256 devices in a mesh: dp: 8 (over x, z_hi), ts: 32 (over z_lo, y, core).
Axes of the slice: x: 4, y: 4, z: 8 (z_hi: 2, z_lo: 4; z = z_hi * 4 + z_lo), core: 2. Of those that a mesh axis runs over, the one named last changes fastest.
Arguments:
- clip_video: bfloat16 [512, 4, 40, 128], P(('dp', 'ts')), may hold values from -6 to 6
- conv_weight: bfloat16 [3, 3, 3, 128, 128], replicated, may hold values from -0.109375 to 0.109375
- embed_weight: bfloat16 [128, 5120], replicated, may hold values from -0.5 to 0.5
- gain_spatial: float32 [5120], replicated, may hold values from 0.5 to 1.5
- gain_temporal: float32 [5120], replicated, may hold values from 0.5 to 1.5
- input_spatial: bfloat16 [5120, 384], P(('dp', 'ts')), may hold values from -0.078125 to 0.078125
- input_temporal: bfloat16 [5120, 384], P(('dp', 'ts')), may hold values from -0.078125 to 0.078125
- output_spatial: bfloat16 [128, 5120], replicated, may hold values from -2 to 2
- output_temporal: bfloat16 [128, 5120], replicated, may hold values from -2 to 2
- cotangent: bfloat16 [512, 4, 40, 5120], P(('dp', 'ts')), may hold values from -6 to 6
Outputs:
- layer_output: bfloat16 [512, 4, 40, 5120], P(('dp', 'ts'))
- grad_spatial: float32 [5120, 384], P(('dp', 'ts'))
The draws below stay inside these ranges and needn't reach their ends.
All inputs are finite; a program needn't handle non-finite values.
Results may differ from the reference program's by a relative error of at most 0.015.
Values may be sent and summed in bfloat16 or wider, within the bound.
No kernel may reach another device: no remote copies, remote signals or barrier semaphores. Data moves between devices by JAX's collectives and lax.ppermute only.
A program may use at most 128 MiB of HBM per device.

```python
import jax
import jax.numpy as jnp
from jax import lax

D = 5120
HEAD = 128
CH = 128
FR = 16
H = 4
WC = 40
FRAMES = 512
N_DP = 8


def level_of(stream_key, extent, shards, least, largest):
    def one(position, blocks):
        heights = jax.random.uniform(jax.random.fold_in(jax.random.fold_in(stream_key, 6), position), (blocks,), jnp.float32, least / len(shards), largest / len(shards))
        return jnp.repeat(jnp.exp(heights), extent[position] // blocks).reshape((-1,) + (1,) * (len(extent) - position - 1))

    level = one(*shards[0])
    for cut in shards[1:]:
        level = level * one(*cut)
    return level


def bell_draw(stream_key, extent, scale, limit, split=(), dtype=jnp.bfloat16):
    factor_of = level_of(stream_key, extent, split, -0.22, 0.18) if split else 1.0
    drawn = jax.random.normal(stream_key, extent, jnp.float32) * scale * factor_of
    return jnp.minimum(jnp.maximum(drawn, -limit), limit).astype(dtype)


def setup_inputs(seed: int = 0) -> dict:
    keys = jax.random.split(jax.random.key(seed), 11)
    clip_video = bell_draw(keys[0], (FRAMES, H, WC, CH), 1.0, 6.0, ((0, 256),))
    conv_weight = bell_draw(keys[1], (3, 3, 3, CH, CH), (27 * CH) ** -0.5, 0.109375)
    embed_weight = bell_draw(keys[2], (CH, D), CH ** -0.5, 0.5)
    gain_spatial = jnp.clip(1.0 + 0.1 * jax.random.normal(keys[3], (D,), jnp.float32), 0.5, 1.5)
    gain_temporal = jnp.clip(1.0 + 0.1 * jax.random.normal(keys[4], (D,), jnp.float32), 0.5, 1.5)
    input_spatial = bell_draw(keys[5], (D, 3 * HEAD), D ** -0.5, 0.078125, ((0, 256),))
    input_temporal = bell_draw(keys[6], (D, 3 * HEAD), D ** -0.5, 0.078125, ((0, 256),))
    output_spatial = bell_draw(keys[7], (HEAD, D), (HEAD // 16) ** -0.5, 2.0)
    output_temporal = bell_draw(keys[8], (HEAD, D), (HEAD // 16) ** -0.5, 2.0)
    cotangent = bell_draw(keys[9], (FRAMES, H, WC, D), 1.0, 6.0, ((0, 256),))
    return {"clip_video": clip_video, "conv_weight": conv_weight, "embed_weight": embed_weight, "gain_spatial": gain_spatial, "gain_temporal": gain_temporal, "input_spatial": input_spatial, "input_temporal": input_temporal, "output_spatial": output_spatial, "output_temporal": output_temporal, "cotangent": cotangent}


epsilon = 1e-06
masked = -1e+30

def widen(array):
    return lax.optimization_barrier(array).astype(jnp.float32)

def conv_clips(video, weight):
    frames, height, columns, channels = video.shape
    out_channels = weight.shape[-1]
    volume = jnp.pad(video, ((2, 0), (1, 1), (1, 1), (0, 0)))
    summed = jnp.zeros((frames * height * columns, out_channels), jnp.float32)
    for time_tap in range(3):
        for row_tap in range(3):
            for col_tap in range(3):
                window = volume[2 - time_tap:2 - time_tap + frames, row_tap:row_tap + height, col_tap:col_tap + columns, :]
                summed = summed + jnp.dot(window.reshape(-1, channels), weight[time_tap, row_tap, col_tap], preferred_element_type=jnp.float32)
    return summed.reshape(frames, height, columns, out_channels)

def rms_norm(hidden, norm_gain):
    widened = hidden.astype(jnp.float32)
    factor = lax.rsqrt(lax.optimization_barrier(jnp.mean(widened * widened, axis=-1, keepdims=True)) + epsilon)
    return ((widened * factor * norm_gain).astype(jnp.bfloat16), factor)

def rms_norm_grad(hidden, norm_gain, factor, upstream):
    widened = hidden.astype(jnp.float32)
    scaled = upstream * norm_gain
    inner_mean = lax.optimization_barrier(jnp.mean(widened * scaled, axis=-1, keepdims=True))
    return factor * scaled - widened * factor ** 3 * inner_mean

def frame_forward(packed):
    frames, places, triple = packed.shape
    head_size = triple // 3
    flattened = widen(packed)
    queries = flattened[..., :head_size]
    key_rows = flattened[..., head_size:2 * head_size]
    values = flattened[..., 2 * head_size:]
    scores = jnp.einsum('fqd,fkd->fqk', queries, key_rows) * head_size ** (-0.5)
    attend = jax.nn.softmax(scores, axis=-1)
    rounded = widen(attend.astype(jnp.bfloat16))
    mixture = jnp.einsum('fqk,fkd->fqd', rounded, values)
    return (mixture.astype(jnp.bfloat16), attend)

def frame_backward(packed, attend, upstream):
    frames, places, triple = packed.shape
    head_size = triple // 3
    scale_factor = head_size ** (-0.5)
    flattened = widen(packed)
    queries = flattened[..., :head_size]
    key_rows = flattened[..., head_size:2 * head_size]
    values = flattened[..., 2 * head_size:]
    grad_out = widen(upstream)
    rounded = widen(attend.astype(jnp.bfloat16))
    grad_attend = jnp.einsum('fqd,fkd->fqk', grad_out, values)
    grad_values = jnp.einsum('fqk,fqd->fkd', rounded, grad_out)
    grad_scores = attend * (grad_attend - lax.optimization_barrier(jnp.sum(grad_attend * attend, axis=-1, keepdims=True)))
    grad_rounded = widen(grad_scores.astype(jnp.bfloat16))
    grad_queries = jnp.einsum('fqk,fkd->fqd', grad_rounded, key_rows) * scale_factor
    grad_keys = jnp.einsum('fqk,fqd->fkd', grad_rounded, queries) * scale_factor
    joined = jnp.concatenate([grad_queries, grad_keys, grad_values], axis=-1)
    return joined.astype(jnp.bfloat16)

def clip_forward(packed):
    frames, places, triple = packed.shape
    head_size = triple // 3
    volume = widen(packed.reshape(frames // FR, FR, places, triple))
    queries = volume[..., :head_size]
    key_rows = volume[..., head_size:2 * head_size]
    values = volume[..., 2 * head_size:]
    scores = jnp.einsum('cqpd,ckpd->cpqk', queries, key_rows) * head_size ** (-0.5)
    allowed = jnp.arange(FR)[:, None] >= jnp.arange(FR)[None, :]
    scores = jnp.where(allowed, scores, masked)
    attend = jax.nn.softmax(scores, axis=-1)
    rounded = widen(attend.astype(jnp.bfloat16))
    mixture = jnp.einsum('cpqk,ckpd->cqpd', rounded, values)
    return (mixture.astype(jnp.bfloat16).reshape(frames, places, head_size), attend)

def clip_backward(packed, attend, upstream):
    frames, places, triple = packed.shape
    head_size = triple // 3
    scale_factor = head_size ** (-0.5)
    volume = widen(packed.reshape(frames // FR, FR, places, triple))
    queries = volume[..., :head_size]
    key_rows = volume[..., head_size:2 * head_size]
    values = volume[..., 2 * head_size:]
    grad_out = widen(upstream.reshape(frames // FR, FR, places, head_size))
    rounded = widen(attend.astype(jnp.bfloat16))
    grad_attend = jnp.einsum('cqpd,ckpd->cpqk', grad_out, values)
    grad_values = jnp.einsum('cpqk,cqpd->ckpd', rounded, grad_out)
    grad_scores = attend * (grad_attend - lax.optimization_barrier(jnp.sum(grad_attend * attend, axis=-1, keepdims=True)))
    grad_rounded = widen(grad_scores.astype(jnp.bfloat16))
    grad_queries = jnp.einsum('cpqk,ckpd->cqpd', grad_rounded, key_rows) * scale_factor
    grad_keys = jnp.einsum('cpqk,cqpd->ckpd', grad_rounded, queries) * scale_factor
    joined = jnp.concatenate([grad_queries, grad_keys, grad_values], axis=-1)
    return joined.astype(jnp.bfloat16).reshape(frames, places, triple)

def reference(clip_video, conv_weight, embed_weight, gain_spatial, gain_temporal, input_spatial, input_temporal, output_spatial, output_temporal, cotangent):

    def group_pass(grad_first, inputs):
        group_video, group_cotangent = inputs
        features = jax.nn.gelu(conv_clips(group_video, conv_weight), approximate=True).astype(jnp.bfloat16)
        frames, height, columns, channels = features.shape
        places = height * columns
        tokens = frames * places
        embedded = jnp.dot(features.reshape(tokens, channels), embed_weight, preferred_element_type=jnp.float32).astype(jnp.bfloat16)
        normed_one, factor_one = rms_norm(embedded, gain_spatial)
        packed_one = jnp.dot(normed_one, input_spatial, preferred_element_type=jnp.float32).astype(jnp.bfloat16)
        packed_one = packed_one.reshape(frames, places, -1)
        mixture_one, attend_one = frame_forward(packed_one)
        after_space = (embedded.astype(jnp.float32) + jnp.dot(mixture_one.reshape(tokens, -1), output_spatial, preferred_element_type=jnp.float32)).astype(jnp.bfloat16)
        normed_two, factor_two = rms_norm(after_space, gain_temporal)
        packed_two = jnp.dot(normed_two, input_temporal, preferred_element_type=jnp.float32).astype(jnp.bfloat16)
        packed_two = packed_two.reshape(frames, places, -1)
        mixture_two, attend_two = clip_forward(packed_two)
        after_time = (after_space.astype(jnp.float32) + jnp.dot(mixture_two.reshape(tokens, -1), output_temporal, preferred_element_type=jnp.float32)).astype(jnp.bfloat16)
        cotangent_rows = group_cotangent.reshape(tokens, -1)
        grad_mix_two = jnp.dot(cotangent_rows, output_temporal.T, preferred_element_type=jnp.float32).astype(jnp.bfloat16)
        grad_packed_two = clip_backward(packed_two, attend_two, grad_mix_two.reshape(frames, places, -1)).reshape(tokens, -1)
        grad_normed_two = jnp.dot(grad_packed_two, input_temporal.T, preferred_element_type=jnp.float32)
        grad_after = (cotangent_rows.astype(jnp.float32) + rms_norm_grad(after_space, gain_temporal, factor_two, grad_normed_two)).astype(jnp.bfloat16)
        grad_mix_one = jnp.dot(grad_after, output_spatial.T, preferred_element_type=jnp.float32).astype(jnp.bfloat16)
        grad_packed_one = frame_backward(packed_one, attend_one, grad_mix_one.reshape(frames, places, -1)).reshape(tokens, -1)
        grad_first = grad_first + lax.dot_general(normed_one, grad_packed_one, (((0,), (0,)), ((), ())), preferred_element_type=jnp.float32)
        return (grad_first, after_time.reshape(frames, height, columns, -1))
    group_frames = clip_video.shape[0] // N_DP
    stacked_video = clip_video.reshape((N_DP, group_frames) + clip_video.shape[1:])
    stacked_cotangent = cotangent.reshape((N_DP, group_frames) + cotangent.shape[1:])
    zeros_grad = jnp.zeros(input_spatial.shape, jnp.float32)
    total, outputs = lax.scan(group_pass, zeros_grad, (stacked_video, stacked_cotangent))
    return (outputs.reshape(cotangent.shape), total)
```

```python
import jax
import jax.numpy as jnp
from jax import lax
from jax.experimental import pallas as pl
from jax.experimental.pallas import tpu as pltpu
from jax.sharding import Mesh
from jax.sharding import PartitionSpec as P

FR = 16
epsilon = 1e-06
masked = -1e30
f32 = jnp.float32
bf16 = jnp.bfloat16

TS = ("z1", "z0", "y", "c")
ROWS = ("z0", "y", "c")
REST = ("x", "zh", "z1")
CLIP = ("y", "c")
ALL = ("x", "zh", "z1", "z0", "y", "c")


def nt(a, b, **kw):
    return lax.dot_general(a, b, (((1,), (1,)), ((), ())), preferred_element_type=f32, **kw)


def tn(a, b, **kw):
    return lax.dot_general(a, b, (((0,), (0,)), ((), ())), preferred_element_type=f32, **kw)


def nn(a, b, **kw):
    return lax.dot_general(a, b, (((1,), (0,)), ((), ())), preferred_element_type=f32, **kw)


def exchange(parts, axes):
    return lax.all_to_all(parts, axes, 0, 0, tiled=True)


def to_all(value, axes):
    size = 1
    for a in axes:
        size *= lax.axis_size(a)
    return exchange(jnp.broadcast_to(value, (size,) + value.shape), axes)


def conv_local(volume, weight, count):
    frames, height, columns, channels = volume.shape
    out_channels = weight.shape[-1]
    padded = jnp.pad(volume, ((0, 0), (1, 1), (1, 1), (0, 0)))
    summed = jnp.zeros((count * height * columns, out_channels), f32)
    for time_tap in range(3):
        for row_tap in range(3):
            for col_tap in range(3):
                window = padded[
                    2 - time_tap : 2 - time_tap + count,
                    row_tap : row_tap + height,
                    col_tap : col_tap + columns,
                    :,
                ]
                summed = summed + nn(
                    window.reshape(-1, channels), weight[time_tap, row_tap, col_tap]
                )
    return summed


def products_kernel(e_ref, os_ref, ot_ref, cot_ref, gram_ref, cots_ref, cott_ref):
    @pl.when(pl.program_id(0) == 0)
    def _():
        gram_ref[...] = jnp.zeros_like(gram_ref)
        cots_ref[...] = jnp.zeros_like(cots_ref)
        cott_ref[...] = jnp.zeros_like(cott_ref)

    e, o, t, c = e_ref[...], os_ref[...], ot_ref[...], cot_ref[...]
    both = jnp.concatenate([e, o], axis=0)
    gram_ref[...] += nt(both, both)
    cots_ref[...] += nt(c, o)
    cott_ref[...] += nt(c, t)


def products(embed, out_s, out_t, cot):
    width = embed.shape[1]
    head = embed.shape[0]
    tokens = cot.shape[0]
    block = 1024
    row = lambda rows: pl.BlockSpec((rows, block), lambda i: (0, i))
    full = lambda r, c: pl.BlockSpec((r, c), lambda i: (0, 0))
    return pl.pallas_call(
        products_kernel,
        grid=(width // block,),
        in_specs=[row(head), row(head), row(head), row(tokens)],
        out_specs=[full(2 * head, 2 * head), full(tokens, head), full(tokens, head)],
        out_shape=[
            jax.ShapeDtypeStruct((2 * head, 2 * head), f32),
            jax.ShapeDtypeStruct((tokens, head), f32),
            jax.ShapeDtypeStruct((tokens, head), f32),
        ],
        name="products",
    )(embed, out_s, out_t, cot)


def output_kernel(f_ref, m_ref, t_ref, e_ref, os_ref, ot_ref, out_ref):
    total = nn(f_ref[...], e_ref[...]) + nn(m_ref[...], os_ref[...]) + nn(t_ref[...], ot_ref[...])
    out_ref[...] = total.astype(bf16)


def output_rows(feats, mix_s, mix_t, embed, out_s, out_t):
    tokens, head = feats.shape
    width = embed.shape[1]
    block = 1024
    row = lambda rows: pl.BlockSpec((rows, block), lambda i: (0, i))
    full = pl.BlockSpec((tokens, head), lambda i: (0, 0))
    return pl.pallas_call(
        output_kernel,
        grid=(width // block,),
        in_specs=[full, full, full, row(head), row(head), row(head)],
        out_specs=row(tokens),
        out_shape=jax.ShapeDtypeStruct((tokens, width), bf16),
        name="output_rows",
    )(feats, mix_s, mix_t, embed, out_s, out_t)


def softmax_rows(scores):
    top = jnp.max(scores, axis=-1, keepdims=True)
    raised = jnp.exp(scores - top)
    return raised / jnp.sum(raised, axis=-1, keepdims=True)


def shards(
    clip_video,
    conv_weight,
    embed_weight,
    gain_spatial,
    gain_temporal,
    input_spatial,
    input_temporal,
    output_spatial,
    output_temporal,
    cotangent,
):
    frames, height, columns, channels = clip_video.shape
    places = height * columns
    tokens = frames * places
    head = embed_weight.shape[0]
    width = embed_weight.shape[1]
    triple = 3 * head
    rows_here = input_spatial.shape[0]
    n_rows = 1
    for a in ROWS:
        n_rows *= lax.axis_size(a)
    cols = triple // n_rows
    scale = head**-0.5
    exact = dict(precision=lax.Precision.HIGHEST)

    n_ts = 1
    for a in TS:
        n_ts *= lax.axis_size(a)
    prior = lax.ppermute(clip_video, TS, [(i, i + 1) for i in range(n_ts - 1)])

    both = jnp.concatenate(
        [input_spatial.reshape(rows_here, n_rows, cols), input_temporal.reshape(rows_here, n_rows, cols)],
        axis=-1,
    )
    mine = exchange(jnp.moveaxis(both, 1, 0), ROWS).reshape(n_rows * rows_here, 2 * cols)
    start = lax.axis_index(REST) * (n_rows * rows_here)
    e_cut = lax.dynamic_slice_in_dim(embed_weight, start, n_rows * rows_here, 1).astype(f32)
    o_cut = lax.dynamic_slice_in_dim(output_spatial, start, n_rows * rows_here, 1).astype(f32)
    gs_cut = lax.dynamic_slice_in_dim(gain_spatial, start, n_rows * rows_here, 0)
    gt_cut = lax.dynamic_slice_in_dim(gain_temporal, start, n_rows * rows_here, 0)
    w_s = mine[:, :cols].astype(f32) * gs_cut[:, None]
    w_t = mine[:, cols:].astype(f32) * gt_cut[:, None]
    dims = (((0,), (1,)), ((), ()))
    part = jnp.concatenate(
        [
            lax.dot_general(w_s, e_cut, dims, preferred_element_type=f32, **exact),
            lax.dot_general(w_t, e_cut, dims, preferred_element_type=f32, **exact),
            lax.dot_general(w_t, o_cut, dims, preferred_element_type=f32, **exact),
        ],
        axis=0,
    ).astype(bf16)
    piece = to_all(part, REST).astype(f32).sum(axis=0).astype(bf16)
    pieces = to_all(piece, ROWS)
    map_s = pieces[:, :cols].reshape(triple, head)
    map_te = pieces[:, cols : 2 * cols].reshape(triple, head)
    map_to = pieces[:, 2 * cols :].reshape(triple, head)

    volume = jnp.concatenate([prior, clip_video], axis=0)
    feats = jax.nn.gelu(conv_local(volume, conv_weight, frames), approximate=True).astype(bf16)
    gram, cot_s, cot_t = products(
        embed_weight, output_spatial, output_temporal, cotangent.reshape(tokens, width)
    )
    gram = gram * (1.0 / width)
    wide = feats.astype(f32)
    square = jnp.sum(nn(wide, gram[:head, :head], **exact) * wide, axis=-1, keepdims=True)
    factor_one = lax.rsqrt(square + epsilon)

    packed = (nt(feats, map_s) * factor_one).astype(bf16).reshape(frames, places, triple)
    q, k, v = packed[..., :head], packed[..., head : 2 * head], packed[..., 2 * head :]
    scores = jnp.einsum("fqd,fkd->fqk", q, k, preferred_element_type=f32) * scale
    attend = softmax_rows(scores)
    rounded = attend.astype(bf16)
    mix = jnp.einsum("fqk,fkd->fqd", rounded, v, preferred_element_type=f32).astype(bf16)

    sent = jnp.concatenate(
        [feats.reshape(frames, places, head), mix, cot_t.astype(bf16).reshape(frames, places, head)],
        axis=-1,
    )
    got = lax.all_to_all(sent, CLIP, split_axis=1, concat_axis=0, tiled=True)
    spots = got.shape[1]
    got = got.reshape(FR * spots, triple)
    x = got[:, : 2 * head]
    g = got[:, 2 * head :]
    xw = x.astype(f32)
    xg = nn(xw, gram, **exact)
    factor_two = lax.rsqrt(jnp.sum(xg * xw, axis=-1, keepdims=True) + epsilon)
    raw = nt(x[:, :head], map_te) + nt(x[:, head:], map_to)
    packed_t = (raw * factor_two).astype(bf16)
    qt, kt, vt = packed_t[:, :head], packed_t[:, head : 2 * head], packed_t[:, 2 * head :]
    n = FR * spots
    row = lax.broadcasted_iota(jnp.int32, (n, n), 0)
    col = lax.broadcasted_iota(jnp.int32, (n, n), 1)
    allowed = (row >= col) & (row % spots == col % spots)
    att_t = softmax_rows(jnp.where(allowed, nt(qt, kt) * scale, masked))
    rnd_t = att_t.astype(bf16)
    mix_t = nn(rnd_t, vt).astype(bf16)
    d_att = nt(g, vt)
    d_v = tn(rnd_t, g)
    d_sc = (att_t * (d_att - jnp.sum(d_att * att_t, axis=-1, keepdims=True))).astype(bf16)
    d_q = nn(d_sc, kt) * scale
    d_k = tn(d_sc, qt) * scale
    gpt = jnp.concatenate([d_q, d_k, d_v], axis=-1).astype(bf16)
    inner = jnp.sum(gpt.astype(f32) * raw, axis=-1, keepdims=True) * (1.0 / width)
    corr = factor_two * nn(gpt, map_to) - (factor_two**3 * inner * width) * xg[:, head:]
    back = jnp.concatenate([mix_t, corr.astype(bf16)], axis=-1).reshape(FR, spots, 2 * head)
    home = lax.all_to_all(back, CLIP, split_axis=0, concat_axis=1, tiled=True)
    home = home.reshape(tokens, 2 * head)
    mix_home = home[:, :head]

    up = (cot_s + home[:, head:].astype(f32)).astype(bf16).reshape(frames, places, head)
    d_att = jnp.einsum("fqd,fkd->fqk", up, v, preferred_element_type=f32)
    d_v = jnp.einsum("fqk,fqd->fkd", rounded, up, preferred_element_type=f32)
    d_sc = (attend * (d_att - jnp.sum(d_att * attend, axis=-1, keepdims=True))).astype(bf16)
    d_q = jnp.einsum("fqk,fkd->fqd", d_sc, k, preferred_element_type=f32) * scale
    d_k = jnp.einsum("fqk,fqd->fkd", d_sc, q, preferred_element_type=f32) * scale
    gps = jnp.concatenate([d_q, d_k, d_v], axis=-1).astype(bf16).reshape(tokens, triple)
    total = tn(gps, (wide * factor_one).astype(bf16)).astype(bf16)
    total = exchange(total.reshape(n_rows, cols, head), ROWS).astype(f32).sum(axis=0).astype(bf16)
    total = to_all(total, REST).astype(f32).sum(axis=0).astype(bf16)
    total = to_all(total, ROWS).reshape(triple, head)
    first = lax.axis_index(ALL) * rows_here
    e_mine = lax.dynamic_slice_in_dim(embed_weight, first, rows_here, 1)
    g_mine = lax.dynamic_slice_in_dim(gain_spatial, first, rows_here, 0)
    grad = lax.dot_general(e_mine, total, (((0,), (1,)), ((), ())), preferred_element_type=f32)
    grad = grad * g_mine[:, None]

    layer = output_rows(
        feats, mix.reshape(tokens, head), mix_home, embed_weight, output_spatial, output_temporal
    )
    return (layer.reshape(frames, height, columns, width), grad)


def solution(mesh):
    split = Mesh(mesh.devices.reshape(4, 2, 2, 2, 4, 2), ALL)
    rows = P(ALL, None)
    blocks = P(ALL, None, None, None)
    placed = (blocks, P(), P(), P(), P(), rows, rows, P(), P(), blocks)
    return jax.shard_map(
        shards,
        mesh=split,
        in_specs=placed,
        out_specs=(blocks, rows),
        check_vma=False,
    )
```

```python
import jax
import jax.numpy as jnp
from jax import lax
from jax.experimental import pallas as pl
from jax.experimental.pallas import tpu as pltpu
from jax.sharding import Mesh
from jax.sharding import PartitionSpec as P

FR = 16
epsilon = 1e-06
masked = -1e30
f32 = jnp.float32
bf16 = jnp.bfloat16

ALL = ("x", "zh", "zl", "y", "c")
TS = ("zl", "y", "c")
DP = ("x", "zh")
PLANE = ("x", "y", "c")
LINE = ("zh", "zl")
CLIP = ("y", "c")


def nt(a, b, **kw):
    return lax.dot_general(a, b, (((1,), (1,)), ((), ())), preferred_element_type=f32, **kw)


def tn(a, b, **kw):
    return lax.dot_general(a, b, (((0,), (0,)), ((), ())), preferred_element_type=f32, **kw)


def nn(a, b, **kw):
    return lax.dot_general(a, b, (((1,), (0,)), ((), ())), preferred_element_type=f32, **kw)


def exchange(parts, axes):
    return lax.all_to_all(parts, axes, 0, 0, tiled=True)


def to_all(value, axes):
    size = 1
    for a in axes:
        size *= lax.axis_size(a)
    return exchange(jnp.broadcast_to(value, (size,) + value.shape), axes)


def conv_local(volume, weight, count):
    frames, height, columns, channels = volume.shape
    out_channels = weight.shape[-1]
    padded = jnp.pad(volume, ((0, 0), (1, 1), (1, 1), (0, 0)))
    summed = jnp.zeros((count * height * columns, out_channels), f32)
    for time_tap in range(3):
        for row_tap in range(3):
            for col_tap in range(3):
                window = padded[
                    2 - time_tap : 2 - time_tap + count,
                    row_tap : row_tap + height,
                    col_tap : col_tap + columns,
                    :,
                ]
                summed = summed + nn(
                    window.reshape(-1, channels), weight[time_tap, row_tap, col_tap]
                )
    return summed


def products_kernel(e_ref, os_ref, ot_ref, cot_ref, gram_ref, cots_ref, cott_ref):
    @pl.when(pl.program_id(0) == 0)
    def _():
        gram_ref[...] = jnp.zeros_like(gram_ref)
        cots_ref[...] = jnp.zeros_like(cots_ref)
        cott_ref[...] = jnp.zeros_like(cott_ref)

    e, o, t, c = e_ref[...], os_ref[...], ot_ref[...], cot_ref[...]
    both = jnp.concatenate([e, o], axis=0)
    gram_ref[...] += nt(both, both)
    cots_ref[...] += nt(c, o)
    cott_ref[...] += nt(c, t)


def products(embed, out_s, out_t, cot):
    width = embed.shape[1]
    head = embed.shape[0]
    tokens = cot.shape[0]
    block = 1024
    row = lambda rows: pl.BlockSpec((rows, block), lambda i: (0, i))
    full = lambda r, c: pl.BlockSpec((r, c), lambda i: (0, 0))
    return pl.pallas_call(
        products_kernel,
        grid=(width // block,),
        in_specs=[row(head), row(head), row(head), row(tokens)],
        out_specs=[full(2 * head, 2 * head), full(tokens, head), full(tokens, head)],
        out_shape=[
            jax.ShapeDtypeStruct((2 * head, 2 * head), f32),
            jax.ShapeDtypeStruct((tokens, head), f32),
            jax.ShapeDtypeStruct((tokens, head), f32),
        ],
        name="products",
    )(embed, out_s, out_t, cot)


def output_kernel(f_ref, m_ref, t_ref, e_ref, os_ref, ot_ref, out_ref):
    total = nn(f_ref[...], e_ref[...]) + nn(m_ref[...], os_ref[...]) + nn(t_ref[...], ot_ref[...])
    out_ref[...] = total.astype(bf16)


def output_rows(feats, mix_s, mix_t, embed, out_s, out_t):
    tokens, head = feats.shape
    width = embed.shape[1]
    block = 1024
    row = lambda rows: pl.BlockSpec((rows, block), lambda i: (0, i))
    full = pl.BlockSpec((tokens, head), lambda i: (0, 0))
    return pl.pallas_call(
        output_kernel,
        grid=(width // block,),
        in_specs=[full, full, full, row(head), row(head), row(head)],
        out_specs=row(tokens),
        out_shape=jax.ShapeDtypeStruct((tokens, width), bf16),
        name="output_rows",
    )(feats, mix_s, mix_t, embed, out_s, out_t)


def maps_kernel(at_ref, ws_ref, wt_ref, e_ref, os_ref, gs_ref, gt_ref, maps_ref, e_mine_ref, g_mine_ref):
    rows, triple = ws_ref.shape
    head, wide = e_ref.shape
    first = at_ref[1] * rows
    r = lax.broadcasted_iota(jnp.int32, (rows, wide), 0)
    c = lax.broadcasted_iota(jnp.int32, (rows, wide), 1)
    chosen = jnp.where(c == r + first, 1.0, 0.0)
    pick = chosen.astype(bf16)
    e = e_ref[...]
    e32 = e.astype(f32)
    o32 = os_ref[...].astype(f32)

    def product(weight, scaled):
        placed = tn(weight, pick).astype(bf16)
        high = scaled.astype(bf16)
        low = (scaled - high.astype(f32)).astype(bf16)
        return nt(placed, high) + nt(placed, low)

    gs = gs_ref[...]
    gt = gt_ref[...]
    maps_ref[:triple] = product(ws_ref[...], e32 * gs).astype(bf16)
    later = product(wt_ref[...], jnp.concatenate([e32, o32], axis=0) * gt)
    maps_ref[triple : 2 * triple] = later[:, :head].astype(bf16)
    maps_ref[2 * triple : 3 * triple] = later[:, head:].astype(bf16)
    maps_ref[3 * triple :] = jnp.zeros((maps_ref.shape[0] - 3 * triple, head), bf16)
    e_mine_ref[...] = nt(pick, e).astype(bf16)
    g_mine_ref[...] = jnp.broadcast_to(jnp.sum(chosen * gs, axis=1, keepdims=True), g_mine_ref.shape)


def local_maps(at, w_s, w_t, embed, out_s, gain_s, gain_t, padded):
    rows, triple = w_s.shape
    head, width = embed.shape
    wide = width // lax.axis_size(DP[0]) // lax.axis_size(DP[1])
    full = lambda r, c: pl.BlockSpec((r, c), lambda i, at: (0, 0))
    cut = lambda r: pl.BlockSpec((r, wide), lambda i, at: (0, at[0]))
    return pl.pallas_call(
        maps_kernel,
        grid_spec=pltpu.PrefetchScalarGridSpec(
            num_scalar_prefetch=1,
            grid=(1,),
            in_specs=[full(rows, triple), full(rows, triple), cut(head), cut(head), cut(1), cut(1)],
            out_specs=[full(padded, head), full(rows, head), full(rows, triple)],
        ),
        out_shape=[
            jax.ShapeDtypeStruct((padded, head), bf16),
            jax.ShapeDtypeStruct((rows, head), bf16),
            jax.ShapeDtypeStruct((rows, triple), f32),
        ],
        name="local_maps",
    )(at, w_s, w_t, embed, out_s, gain_s.reshape(1, width), gain_t.reshape(1, width))


def group_size(axes):
    size = 1
    for a in axes:
        size *= lax.axis_size(a)
    return size


def summed_everywhere(value):
    n = group_size(PLANE)
    parts = exchange(value.reshape(n, value.shape[0] // n, value.shape[1]), PLANE)
    mine = parts.astype(f32).sum(axis=0).astype(bf16)
    mine = to_all(mine, LINE).astype(f32).sum(axis=0).astype(bf16)
    return to_all(mine, PLANE).reshape(value.shape)


def softmax_rows(scores):
    top = jnp.max(scores, axis=-1, keepdims=True)
    raised = jnp.exp(scores - top)
    return raised / jnp.sum(raised, axis=-1, keepdims=True)


def shards(
    clip_video,
    conv_weight,
    embed_weight,
    gain_spatial,
    gain_temporal,
    input_spatial,
    input_temporal,
    output_spatial,
    output_temporal,
    cotangent,
):
    frames, height, columns, channels = clip_video.shape
    places = height * columns
    tokens = frames * places
    head, width = embed_weight.shape
    triple = 3 * head
    scale = head**-0.5
    exact = dict(precision=lax.Precision.HIGHEST)
    n_ts = group_size(TS)
    n_clip = group_size(CLIP)
    spots = places // n_clip
    clip_tokens = FR * places
    own = FR * spots

    prior = lax.ppermute(clip_video, TS, [(i, i + 1) for i in range(n_ts - 1)])

    at = jnp.stack([lax.axis_index(DP), lax.axis_index(TS)]).astype(jnp.int32)
    maps, e_mine, g_mine = local_maps(
        at, input_spatial, input_temporal, embed_weight, output_spatial, gain_spatial, gain_temporal, 10 * head
    )
    maps = summed_everywhere(maps)
    map_s = maps[:triple]
    map_te = maps[triple : 2 * triple]
    map_to = maps[2 * triple : 3 * triple]

    volume = jnp.concatenate([prior, clip_video], axis=0)
    feats_home = jax.nn.gelu(conv_local(volume, conv_weight, frames), approximate=True).astype(bf16)
    feats = to_all(feats_home, CLIP).reshape(FR, places, head)
    gram, cot_s, cot_t = products(
        embed_weight, output_spatial, output_temporal, cotangent.reshape(tokens, width)
    )
    sent = jnp.concatenate([cot_s, cot_t], axis=-1).astype(bf16).reshape(frames, places, 2 * head)
    cots = lax.all_to_all(sent, CLIP, split_axis=1, concat_axis=0, tiled=True)
    gram = gram * (1.0 / width)
    slot = lax.axis_index(CLIP) * spots
    flat = feats.reshape(clip_tokens, head)
    wide = flat.astype(f32)
    square = jnp.sum(nn(wide, gram[:head, :head], **exact) * wide, axis=-1, keepdims=True)
    factor_one = lax.rsqrt(square + epsilon)
    scaled = (wide * factor_one).astype(bf16)
    feats_own = lax.dynamic_slice_in_dim(feats, slot, spots, 1).reshape(own, head)
    scaled_own = lax.dynamic_slice_in_dim(scaled.reshape(FR, places, head), slot, spots, 1).reshape(own, head)
    factor_own = lax.dynamic_slice_in_dim(factor_one.reshape(FR, places, 1), slot, spots, 1).reshape(own, 1)

    q = (nt(feats_own, map_s[:head]) * factor_own).astype(bf16).reshape(FR, spots, head)
    kv = (nt(flat, map_s[head:]) * factor_one).astype(bf16).reshape(FR, places, 2 * head)
    k, v = kv[..., :head], kv[..., head:]
    scores = jnp.einsum("fqd,fkd->fqk", q, k, preferred_element_type=f32) * scale
    attend = softmax_rows(scores)
    rounded = attend.astype(bf16)
    mix = jnp.einsum("fqk,fkd->fqd", rounded, v, preferred_element_type=f32).astype(bf16)

    mix_own = mix.reshape(own, head)
    g = cots[..., head:].reshape(own, head)
    x = jnp.concatenate([feats_own, mix_own], axis=-1)
    xw = x.astype(f32)
    xg = nn(xw, gram, **exact)
    factor_two = lax.rsqrt(jnp.sum(xg * xw, axis=-1, keepdims=True) + epsilon)
    raw = nt(feats_own, map_te) + nt(mix_own, map_to)
    packed_t = (raw * factor_two).astype(bf16)
    qt, kt, vt = packed_t[:, :head], packed_t[:, head : 2 * head], packed_t[:, 2 * head :]
    row = lax.broadcasted_iota(jnp.int32, (own, own), 0)
    col = lax.broadcasted_iota(jnp.int32, (own, own), 1)
    allowed = (row >= col) & (row % spots == col % spots)
    att_t = softmax_rows(jnp.where(allowed, nt(qt, kt) * scale, masked))
    rnd_t = att_t.astype(bf16)
    mix_t = nn(rnd_t, vt).astype(bf16)
    d_att = nt(g, vt)
    d_v = tn(rnd_t, g)
    d_sc = (att_t * (d_att - jnp.sum(d_att * att_t, axis=-1, keepdims=True))).astype(bf16)
    d_q = nn(d_sc, kt) * scale
    d_k = tn(d_sc, qt) * scale
    gpt = jnp.concatenate([d_q, d_k, d_v], axis=-1).astype(bf16)
    inner = jnp.sum(gpt.astype(f32) * raw, axis=-1, keepdims=True)
    corr = factor_two * nn(gpt, map_to) - (factor_two**3 * inner) * xg[:, head:]

    up = (cots[..., :head].astype(f32) + corr.reshape(FR, spots, head)).astype(bf16)
    d_att = jnp.einsum("fqd,fkd->fqk", up, v, preferred_element_type=f32)
    d_v = jnp.einsum("fqk,fqd->fkd", rounded, up, preferred_element_type=f32).astype(bf16)
    d_sc = (attend * (d_att - jnp.sum(d_att * attend, axis=-1, keepdims=True))).astype(bf16)
    d_q = (jnp.einsum("fqk,fkd->fqd", d_sc, k, preferred_element_type=f32) * scale).astype(bf16)
    d_k = (jnp.einsum("fqk,fqd->fkd", d_sc, q, preferred_element_type=f32) * scale).astype(bf16)
    total = jnp.concatenate(
        [
            tn(d_q.reshape(own, head), scaled_own),
            tn(d_k.reshape(clip_tokens, head), scaled),
            tn(d_v.reshape(clip_tokens, head), scaled),
            jnp.zeros((head, head), f32),
        ],
        axis=0,
    ).astype(bf16)
    total = summed_everywhere(total)[:triple]
    grad = nt(e_mine, total) * g_mine

    back = jnp.concatenate([mix, mix_t.reshape(FR, spots, head)], axis=-1)
    home = lax.all_to_all(back, CLIP, split_axis=0, concat_axis=1, tiled=True).reshape(tokens, 2 * head)
    layer = output_rows(
        feats_home, home[:, :head], home[:, head:], embed_weight, output_spatial, output_temporal
    )
    return (layer.reshape(frames, height, columns, width), grad)


def solution(mesh):
    split = Mesh(mesh.devices.reshape(4, 2, 4, 4, 2), ALL)
    rows = P(ALL, None)
    blocks = P(ALL, None, None, None)
    placed = (blocks, P(), P(), P(), P(), rows, rows, P(), P(), blocks)
    return jax.shard_map(
        shards,
        mesh=split,
        in_specs=placed,
        out_specs=(blocks, rows),
        check_vma=False,
    )
```

```python
import jax
import jax.numpy as jnp
from jax import lax
from jax.experimental import pallas as pl
from jax.experimental.pallas import tpu as pltpu
from jax.sharding import Mesh
from jax.sharding import PartitionSpec as P

FR = 16
epsilon = 1e-06
masked = -1e30
f32 = jnp.float32
bf16 = jnp.bfloat16

ALL = ("x", "zh", "zl", "y", "c")
TS = ("zl", "y", "c")
DP = ("x", "zh")
PLANE = ("x", "y", "c")
LINE = ("zh", "zl")
CLIP = ("y", "c")


def nt(a, b, **kw):
    return lax.dot_general(a, b, (((1,), (1,)), ((), ())), preferred_element_type=f32, **kw)


def tn(a, b, **kw):
    return lax.dot_general(a, b, (((0,), (0,)), ((), ())), preferred_element_type=f32, **kw)


def nn(a, b, **kw):
    return lax.dot_general(a, b, (((1,), (0,)), ((), ())), preferred_element_type=f32, **kw)


def exchange(parts, axes):
    return lax.all_to_all(parts, axes, 0, 0, tiled=True)


def to_all(value, axes):
    size = 1
    for a in axes:
        size *= lax.axis_size(a)
    return exchange(jnp.broadcast_to(value, (size,) + value.shape), axes)


def conv_local(volume, weight, count):
    _, height, columns, channels = volume.shape
    out_channels = weight.shape[-1]
    padded = jnp.pad(volume, ((0, 0), (1, 1), (1, 1), (0, 0)))
    summed = jnp.zeros((count * height * columns, out_channels), f32)
    for time_tap in range(3):
        for row_tap in range(3):
            for col_tap in range(3):
                window = padded[
                    2 - time_tap : 2 - time_tap + count,
                    row_tap : row_tap + height,
                    col_tap : col_tap + columns,
                    :,
                ]
                summed = summed + nn(
                    window.reshape(-1, channels), weight[time_tap, row_tap, col_tap]
                )
    return summed


def products_kernel(after_ref, e_ref, os_ref, ot_ref, cot_ref, gram_ref, cots_ref, cott_ref):
    @pl.when(pl.program_id(0) == 0)
    def _():
        gram_ref[...] = jnp.zeros_like(gram_ref)
        cots_ref[...] = jnp.zeros_like(cots_ref)
        cott_ref[...] = jnp.zeros_like(cott_ref)

    e, o, t, c = e_ref[...], os_ref[...], ot_ref[...], cot_ref[...]
    both = jnp.concatenate([e, o], axis=0)
    gram_ref[...] += nt(both, both)
    cots_ref[...] += nt(c, o)
    cott_ref[...] += nt(c, t)


def products(after, embed, out_s, out_t, cot):
    width = embed.shape[1]
    head = embed.shape[0]
    tokens = cot.shape[0]
    block = 1024
    row = lambda rows: pl.BlockSpec((rows, block), lambda i: (0, i))
    full = lambda r, c: pl.BlockSpec((r, c), lambda i: (0, 0))
    return pl.pallas_call(
        products_kernel,
        grid=(width // block,),
        in_specs=[full(*after.shape), row(head), row(head), row(head), row(tokens)],
        out_specs=[full(2 * head, 2 * head), full(tokens, head), full(tokens, head)],
        out_shape=[
            jax.ShapeDtypeStruct((2 * head, 2 * head), f32),
            jax.ShapeDtypeStruct((tokens, head), f32),
            jax.ShapeDtypeStruct((tokens, head), f32),
        ],
        name="products",
    )(after, embed, out_s, out_t, cot)


def output_kernel(f_ref, m_ref, t_ref, e_ref, os_ref, ot_ref, out_ref):
    total = nn(f_ref[...], e_ref[...]) + nn(m_ref[...], os_ref[...]) + nn(t_ref[...], ot_ref[...])
    out_ref[...] = total.astype(bf16)


def output_rows(feats, mix_s, mix_t, embed, out_s, out_t):
    tokens, head = feats.shape
    width = embed.shape[1]
    block = 1024
    row = lambda rows: pl.BlockSpec((rows, block), lambda i: (0, i))
    full = pl.BlockSpec((tokens, head), lambda i: (0, 0))
    return pl.pallas_call(
        output_kernel,
        grid=(width // block,),
        in_specs=[full, full, full, row(head), row(head), row(head)],
        out_specs=row(tokens),
        out_shape=jax.ShapeDtypeStruct((tokens, width), bf16),
        name="output_rows",
    )(feats, mix_s, mix_t, embed, out_s, out_t)


def maps_kernel(at_ref, ws_ref, wt_ref, e_ref, os_ref, gs_ref, gt_ref, maps_ref, e_mine_ref, g_mine_ref):
    rows, triple = ws_ref.shape
    head, wide = e_ref.shape
    first = at_ref[1] * rows
    r = lax.broadcasted_iota(jnp.int32, (rows, wide), 0)
    c = lax.broadcasted_iota(jnp.int32, (rows, wide), 1)
    chosen = jnp.where(c == r + first, 1.0, 0.0)
    pick = chosen.astype(bf16)
    e = e_ref[...]
    e32 = e.astype(f32)
    o32 = os_ref[...].astype(f32)

    def product(weight, scaled):
        placed = tn(weight, pick).astype(bf16)
        high = scaled.astype(bf16)
        low = (scaled - high.astype(f32)).astype(bf16)
        return nt(placed, high) + nt(placed, low)

    gs = gs_ref[...]
    gt = gt_ref[...]
    maps_ref[:triple] = product(ws_ref[...], e32 * gs).astype(bf16)
    later = product(wt_ref[...], jnp.concatenate([e32, o32], axis=0) * gt)
    maps_ref[triple : 2 * triple] = later[:, :head].astype(bf16)
    maps_ref[2 * triple : 3 * triple] = later[:, head:].astype(bf16)
    maps_ref[3 * triple :] = jnp.zeros((maps_ref.shape[0] - 3 * triple, head), bf16)
    e_mine_ref[...] = nt(pick, e).astype(bf16)
    g_mine_ref[...] = jnp.broadcast_to(jnp.sum(chosen * gs, axis=1, keepdims=True), g_mine_ref.shape)


def local_maps(at, w_s, w_t, embed, out_s, gain_s, gain_t, padded):
    rows, triple = w_s.shape
    head, width = embed.shape
    wide = width // lax.axis_size(DP[0]) // lax.axis_size(DP[1])
    full = lambda r, c: pl.BlockSpec((r, c), lambda i, at: (0, 0))
    cut = lambda r: pl.BlockSpec((r, wide), lambda i, at: (0, at[0]))
    return pl.pallas_call(
        maps_kernel,
        grid_spec=pltpu.PrefetchScalarGridSpec(
            num_scalar_prefetch=1,
            grid=(1,),
            in_specs=[full(rows, triple), full(rows, triple), cut(head), cut(head), cut(1), cut(1)],
            out_specs=[full(padded, head), full(rows, head), full(rows, triple)],
        ),
        out_shape=[
            jax.ShapeDtypeStruct((padded, head), bf16),
            jax.ShapeDtypeStruct((rows, head), bf16),
            jax.ShapeDtypeStruct((rows, triple), f32),
        ],
        name="local_maps",
    )(at, w_s, w_t, embed, out_s, gain_s.reshape(1, width), gain_t.reshape(1, width))


def group_size(axes):
    size = 1
    for a in axes:
        size *= lax.axis_size(a)
    return size


def scattered(value):
    n = group_size(PLANE)
    parts = exchange(value.reshape(n, value.shape[0] // n, value.shape[1]), PLANE)
    return parts.astype(f32).sum(axis=0).astype(bf16)


def gathered(mine, shape):
    parts = to_all(mine, LINE)
    mine = parts.astype(f32).sum(axis=0).astype(bf16)
    return to_all(mine, PLANE).reshape(shape)


def softmax_rows(scores):
    top = jnp.max(scores, axis=-1, keepdims=True)
    raised = jnp.exp(scores - top)
    return raised / jnp.sum(raised, axis=-1, keepdims=True)


def attend_kernel(
    at_ref, flat_ref, scaled_ref, gram_ref, cots_ref, maps_ref,
    total_ref, mix_ref, mix_t_ref, qkv_ref, att_ref, dkv_ref, up_ref, score_ref, rounded_ref, slope_ref,
):
    frames = FR
    head = flat_ref.shape[1]
    places = flat_ref.shape[0] // frames
    pad = mix_ref.shape[0] // frames
    triple = 3 * head
    own = frames * pad
    scale = head**-0.5
    line, core, slot, spots = at_ref[0], at_ref[1], at_ref[2], at_ref[3]

    qkv_ref[...] = nt(scaled_ref[...], maps_ref[:triple]).astype(bf16)
    r = lax.broadcasted_iota(jnp.int32, (pad, places), 0)
    c = lax.broadcasted_iota(jnp.int32, (pad, places), 1)
    pick = jnp.where((c == r + slot) & (r < spots), 1.0, 0.0).astype(bf16)

    feats_own, scaled_own, queries = [], [], []
    for f in range(frames):
        here = slice(f * places, (f + 1) * places)
        both = jnp.concatenate([flat_ref[here], scaled_ref[here], qkv_ref[here, :head]], axis=1)
        got = nn(pick, both).astype(bf16)
        feats_own.append(got[:, :head])
        scaled_own.append(got[:, head : 2 * head])
        queries.append(got[:, 2 * head :])
    for f in range(frames):
        here = slice(f * places, (f + 1) * places)
        score_ref[f * pad : (f + 1) * pad] = nt(queries[f], qkv_ref[here, head : 2 * head])
    att = softmax_rows(score_ref[...] * scale)
    att_ref[...] = att
    rounded_ref[...] = att.astype(bf16)
    for f in range(frames):
        here = slice(f * places, (f + 1) * places)
        mine = slice(f * pad, (f + 1) * pad)
        mix_ref[mine] = nn(rounded_ref[mine], qkv_ref[here, 2 * head :]).astype(bf16)

    feats = jnp.concatenate(feats_own, axis=0)
    mix = mix_ref[...]
    x = jnp.concatenate([feats, mix], axis=1)
    gram = gram_ref[...]
    first = gram.astype(bf16)
    rest = gram - first.astype(f32)
    second = rest.astype(bf16)
    third = (rest - second.astype(f32)).astype(bf16)
    xg = nn(x, first) + (nn(x, second) + nn(x, third))
    factor = lax.rsqrt(jnp.sum(xg * x.astype(f32), axis=-1, keepdims=True) + epsilon)
    map_to = maps_ref[2 * triple : 3 * triple]
    raw = nt(feats, maps_ref[triple : 2 * triple]) + nt(mix, map_to)
    packed = (raw * factor).astype(bf16)
    q, k, v = packed[:, :head], packed[:, head : 2 * head], packed[:, 2 * head :]
    g = jnp.concatenate([cots_ref[i, j, 1] for i in range(2) for j in range(4)], axis=0)

    def spot_frame(shape, dim):
        i = lax.broadcasted_iota(jnp.int32, shape, dim)
        f = i // pad
        other = f // 8
        step = (f // 2) % 4
        number = ((line + 4 - step) % 4) * 4 + (core + other - 2 * core * other) * 2 + f % 2
        return i % pad, number

    row_spot, row_frame = spot_frame((own, 1), 0)
    col_spot, col_frame = spot_frame((1, own), 1)
    allowed = (row_spot == col_spot) & (row_frame >= col_frame)
    att = softmax_rows(jnp.where(allowed, nt(q, k) * scale, masked))
    rounded = att.astype(bf16)
    mix_t_ref[...] = nn(rounded, v).astype(bf16)
    d_att = nt(g, v)
    d_sc = (att * (d_att - jnp.sum(d_att * att, axis=-1, keepdims=True))).astype(bf16)
    d_packed = jnp.concatenate(
        [nn(d_sc, k) * scale, tn(d_sc, q) * scale, tn(rounded, g)], axis=1
    ).astype(bf16)
    inner = jnp.sum(d_packed.astype(f32) * raw, axis=-1, keepdims=True)
    corr = factor * nn(d_packed, map_to) - (factor * factor * factor * inner) * xg[:, head:]
    cot = jnp.concatenate([cots_ref[i, j, 0] for i in range(2) for j in range(4)], axis=0)
    up_ref[...] = (cot.astype(f32) + corr).astype(bf16)

    for f in range(frames):
        here = slice(f * places, (f + 1) * places)
        mine = slice(f * pad, (f + 1) * pad)
        score_ref[mine] = nt(up_ref[mine], qkv_ref[here, 2 * head :])
        dkv_ref[here, head:] = tn(rounded_ref[mine], up_ref[mine]).astype(bf16)
    att = att_ref[...]
    d_att = score_ref[...]
    slope_ref[...] = (att * (d_att - jnp.sum(d_att * att, axis=-1, keepdims=True)) * scale).astype(bf16)
    d_queries = []
    for f in range(frames):
        here = slice(f * places, (f + 1) * places)
        mine = slice(f * pad, (f + 1) * pad)
        slope = slope_ref[mine]
        d_queries.append(nn(slope, qkv_ref[here, head : 2 * head]).astype(bf16))
        dkv_ref[here, :head] = tn(slope, queries[f]).astype(bf16)
    by_query = tn(jnp.concatenate(scaled_own, axis=0), jnp.concatenate(d_queries, axis=0))
    by_key = tn(scaled_ref[...], dkv_ref[...])
    total_ref[:head] = by_query.astype(bf16)
    total_ref[head : 2 * head] = by_key[:, :head].astype(bf16)
    total_ref[2 * head : 3 * head] = by_key[:, head:].astype(bf16)
    total_ref[3 * head :] = jnp.zeros((total_ref.shape[0] - 3 * head, head), bf16)


def attend_all(at, flat, scaled, gram, cots, maps, pad):
    rows, head = flat.shape
    places = rows // FR
    own = FR * pad
    vmem = pl.BlockSpec(memory_space=pltpu.VMEM)
    return pl.pallas_call(
        attend_kernel,
        in_specs=[pl.BlockSpec(memory_space=pltpu.SMEM)] + [vmem] * 5,
        out_specs=[vmem] * 3,
        out_shape=[
            jax.ShapeDtypeStruct((4 * head, head), bf16),
            jax.ShapeDtypeStruct((own, head), bf16),
            jax.ShapeDtypeStruct((own, head), bf16),
        ],
        scratch_shapes=[
            pltpu.VMEM((rows, 3 * head), bf16),
            pltpu.VMEM((own, places), f32),
            pltpu.VMEM((rows, 2 * head), bf16),
            pltpu.VMEM((own, head), bf16),
            pltpu.VMEM((own, places), f32),
            pltpu.VMEM((own, places), bf16),
            pltpu.VMEM((own, places), bf16),
        ],
        name="attend_all",
    )(at, flat, scaled, gram, cots, maps)


def turned(value, axis, step):
    n = lax.axis_size(axis)
    return lax.ppermute(value, axis, [(i, (i + step) % n) for i in range(n)])


def shards(
    clip_video,
    conv_weight,
    embed_weight,
    gain_spatial,
    gain_temporal,
    input_spatial,
    input_temporal,
    output_spatial,
    output_temporal,
    cotangent,
):
    frames, height, columns, _ = clip_video.shape
    places = height * columns
    tokens = frames * places
    head, width = embed_weight.shape
    exact = dict(precision=lax.Precision.HIGHEST)
    n_ts = group_size(TS)
    n_clip = group_size(CLIP)
    spots = places // n_clip
    clip_tokens = FR * places

    prior = lax.ppermute(clip_video, TS, [(i, i + 1) for i in range(n_ts - 1)])

    at = jnp.stack([lax.axis_index(DP), lax.axis_index(TS)]).astype(jnp.int32)
    maps, e_mine, g_mine = local_maps(
        at, input_spatial, input_temporal, embed_weight, output_spatial, gain_spatial, gain_temporal, 10 * head
    )
    prior, g_mine = lax.optimization_barrier((prior, g_mine))
    maps = gathered(scattered(maps), maps.shape)

    volume = jnp.concatenate([prior, clip_video], axis=0)
    feats_home = jax.nn.gelu(conv_local(volume, conv_weight, frames), approximate=True).astype(bf16)
    gram, cot_s, cot_t = products(
        g_mine, embed_weight, output_spatial, output_temporal, cotangent.reshape(tokens, width)
    )
    gram = gram * (1.0 / width)
    n_line = lax.axis_size("y")
    line = lax.axis_index("y")
    core = lax.axis_index("c")
    pad = 32
    cots = jnp.stack([cot_s, cot_t]).astype(bf16).reshape(2, frames, n_line, 2, spots, head)
    cots = jnp.pad(cots, ((0, 0),) * 4 + ((0, pad - spots), (0, 0)))
    cots = cots.transpose(2, 3, 0, 1, 4, 5).reshape(n_line, 4 * frames * pad, head)
    held = [
        jnp.concatenate(
            [feats_home, lax.dynamic_index_in_dim(cots, (line + step) % n_line, 0, keepdims=False)], axis=0
        )
        for step in range(n_line)
    ]
    moved = []
    for step in range(1, n_line):
        moved.append(turned(held[step], "y", step))
    held = jnp.stack([held[0]] + moved)
    feats_near = held[:, :tokens]
    cots_near = held[:, tokens:].reshape(n_line, 2, 2 * frames * pad, head)
    keep = lax.dynamic_index_in_dim(cots_near, core, 1, keepdims=False)
    give = lax.dynamic_index_in_dim(cots_near, 1 - core, 1, keepdims=False)
    other = turned(jnp.concatenate([feats_near, give], axis=1), "c", 1)
    flat = jnp.concatenate([feats_near, other[:, :tokens]], axis=0).reshape(clip_tokens, head)
    cots = jnp.stack([keep, other[:, tokens:]]).reshape(2, n_line, 2, frames * pad, head)
    wide = flat.astype(f32)
    square = jnp.sum(nn(wide, gram[:head, :head], **exact) * wide, axis=-1, keepdims=True)
    scaled = (wide * lax.rsqrt(square + epsilon)).astype(bf16)

    place = jnp.stack([line, core, lax.axis_index(CLIP) * spots, jnp.int32(spots)]).astype(jnp.int32)
    total, mix, mix_t = attend_all(place, flat, scaled, gram, cots, maps, pad)

    share = scattered(total)
    share, mix, mix_t = lax.optimization_barrier((share, mix, mix_t))
    total = gathered(share, total.shape)
    grad = jnp.concatenate([nn(e_mine, total[b * head : (b + 1) * head]) for b in range(3)], axis=1) * g_mine

    back = jnp.concatenate([mix, mix_t], axis=-1).reshape(2, n_line, frames, pad, 2 * head)[:, :, :, :spots]
    moved = []
    for step in range(1, n_line):
        moved.append(turned(back[:, step], "y", -step))
    back = jnp.stack([back[:, 0]] + moved)
    away = turned(back[:, 1], "c", 1)
    home = jnp.stack([back[:, 0], away], axis=1)
    home = jnp.where(core == 0, home, home[:, ::-1])
    home = lax.dynamic_slice_in_dim(jnp.concatenate([home, home], axis=0), (n_line - line) % n_line, n_line, 0)
    home = home.transpose(2, 0, 1, 3, 4).reshape(tokens, 2 * head)
    layer = output_rows(
        feats_home, home[:, :head], home[:, head:], embed_weight, output_spatial, output_temporal
    )
    return (layer.reshape(frames, height, columns, width), grad)


def solution(mesh):
    split = Mesh(mesh.devices.reshape(4, 2, 4, 4, 2), ALL)
    rows = P(ALL, None)
    blocks = P(ALL, None, None, None)
    placed = (blocks, P(), P(), P(), P(), rows, rows, P(), P(), blocks)
    return jax.shard_map(shards, mesh=split, in_specs=placed, out_specs=(blocks, rows), check_vma=False)
```

```python
import jax
import jax.numpy as jnp
from jax import lax
from jax.experimental import pallas as pl
from jax.experimental.pallas import tpu as pltpu
from jax.sharding import Mesh
from jax.sharding import PartitionSpec as P

FR = 16
epsilon = 1e-06
masked = -1e30
f32 = jnp.float32
bf16 = jnp.bfloat16

ALL = ("x", "zh", "zl", "y", "c")
TS = ("zl", "y", "c")
DP = ("x", "zh")
PLANE = ("x", "y", "c")
LINE = ("zh", "zl")
CLIP = ("y", "c")


def nt(a, b, **kw):
    return lax.dot_general(a, b, (((1,), (1,)), ((), ())), preferred_element_type=f32, **kw)


def tn(a, b, **kw):
    return lax.dot_general(a, b, (((0,), (0,)), ((), ())), preferred_element_type=f32, **kw)


def nn(a, b, **kw):
    return lax.dot_general(a, b, (((1,), (0,)), ((), ())), preferred_element_type=f32, **kw)


def exchange(parts, axes):
    return lax.all_to_all(parts, axes, 0, 0, tiled=True)


def to_all(value, axes):
    size = 1
    for a in axes:
        size *= lax.axis_size(a)
    return exchange(jnp.broadcast_to(value, (size,) + value.shape), axes)


def conv_kernel(prior_ref, here_ref, weight_ref, out_ref):
    tokens = here_ref.shape[0]
    columns = here_ref.shape[0] // 8
    volume = jnp.concatenate([prior_ref[...].astype(f32), here_ref[...].astype(f32)], axis=0)
    rows = volume.shape[0]
    place = lax.broadcasted_iota(jnp.int32, (rows, 1), 0) % columns
    left = jnp.where(place == 0, 0.0, pltpu.roll(volume, 1, 0))
    right = jnp.where(place == columns - 1, 0.0, pltpu.roll(volume, rows - 1, 0))
    taps = jnp.concatenate([left, volume, right], axis=1).astype(bf16)
    frame = tokens // 2
    sums = [None, None, None]
    for back in range(3):
        start = (2 - back) * frame
        window = taps[start : start + tokens]
        for up in range(3):
            got = nn(window, weight_ref[back * 3 + up])
            sums[up] = got if sums[up] is None else sums[up] + got
    gap = jnp.zeros((columns, sums[0].shape[1]), f32)
    above, same, below = sums
    for f in range(2):
        lo, hi = f * frame, (f + 1) * frame
        total = (
            same[lo:hi]
            + jnp.concatenate([gap, above[lo : hi - columns]], axis=0)
            + jnp.concatenate([below[lo + columns : hi], gap], axis=0)
        )
        out_ref[lo:hi] = jax.nn.gelu(total, approximate=True).astype(bf16)


def conv_rows(prior, here, weight):
    tokens, channels = here.shape
    vmem = pl.BlockSpec(memory_space=pltpu.VMEM)
    return pl.pallas_call(
        conv_kernel,
        in_specs=[vmem] * 3,
        out_specs=vmem,
        out_shape=jax.ShapeDtypeStruct((tokens, weight.shape[-1]), bf16),
        name="conv_rows",
    )(prior, here, weight.reshape(9, 3 * channels, weight.shape[-1]))


CHUNK = 1024


def products_kernel(
    e_ref, os_ref, ot_ref, cot_ref, gram_ref, cots_ref, weights, cotangents, gram_sum, cots_sum, arrived
):
    head, width = e_ref.shape
    copies = []
    for i in range(width // CHUNK):
        cols = pl.ds(i * CHUNK, CHUNK)
        group = [
            pltpu.make_async_copy(ref.at[:, cols], weights.at[pl.ds(k * head, head), cols], arrived.at[i, k])
            for k, ref in enumerate((e_ref, os_ref, ot_ref))
        ]
        group.append(pltpu.make_async_copy(cot_ref.at[:, cols], cotangents.at[:, cols], arrived.at[i, 3]))
        for copy in group:
            copy.start()
        copies.append(group)
    for i, group in enumerate(copies):
        for copy in group:
            copy.wait()
        cols = slice(i * CHUNK, (i + 1) * CHUNK)
        first = weights[: 2 * head, cols]
        gram = nt(first, first)
        cots = nt(cotangents[:, cols], weights[head:, cols])
        gram_sum[...] = gram if i == 0 else gram_sum[...] + gram
        cots_sum[...] = cots if i == 0 else cots_sum[...] + cots
    gram_ref[...] = gram_sum[...] * (1.0 / width)
    slots, kinds, frames, pad, _ = cots_ref.shape
    places = cots_sum.shape[0] // frames
    spots = places // slots
    r = lax.broadcasted_iota(jnp.int32, (slots * pad, places), 0)
    c = lax.broadcasted_iota(jnp.int32, (slots * pad, places), 1)
    spread = jnp.where((c == (r // pad) * spots + r % pad) & (r % pad < spots), 1.0, 0.0).astype(bf16)
    for f in range(frames):
        got = nn(spread, cots_sum[f * places : (f + 1) * places].astype(bf16)).astype(bf16)
        for slot in range(slots):
            for kind in range(kinds):
                cots_ref[slot, kind, f] = got[slot * pad : (slot + 1) * pad, kind * head : (kind + 1) * head]


def products(embed, out_s, out_t, cot, frames, slots, pad):
    head, width = embed.shape
    tokens = cot.shape[0]
    hbm = pl.BlockSpec(memory_space=pl.ANY)
    vmem = pl.BlockSpec(memory_space=pltpu.VMEM)
    return pl.pallas_call(
        products_kernel,
        in_specs=[hbm] * 4,
        out_specs=[vmem, vmem],
        out_shape=[
            jax.ShapeDtypeStruct((2 * head, 2 * head), f32),
            jax.ShapeDtypeStruct((slots, 2, frames, pad, head), bf16),
        ],
        scratch_shapes=[
            pltpu.VMEM((3 * head, width), bf16),
            pltpu.VMEM((tokens, width), bf16),
            pltpu.VMEM((2 * head, 2 * head), f32),
            pltpu.VMEM((tokens, 2 * head), f32),
            pltpu.SemaphoreType.DMA((width // CHUNK, 4)),
        ],
        name="products",
    )(embed, out_s, out_t, cot)


def output_kernel(f_ref, mixes_ref, e_ref, os_ref, ot_ref, out_ref, weights, rows, arrived, sent):
    head, width = e_ref.shape
    copies = []
    for i in range(width // CHUNK):
        cols = pl.ds(i * CHUNK, CHUNK)
        group = [
            pltpu.make_async_copy(ref.at[:, cols], weights.at[pl.ds(k * head, head), cols], arrived.at[i, k])
            for k, ref in enumerate((e_ref, os_ref, ot_ref))
        ]
        for copy in group:
            copy.start()
        copies.append(group)
    x = jnp.concatenate([f_ref[...], mixes_ref[...]], axis=1)
    leaving = []
    for i, group in enumerate(copies):
        for copy in group:
            copy.wait()
        cols = slice(i * CHUNK, (i + 1) * CHUNK)
        rows[:, cols] = nn(x, weights[:, cols]).astype(bf16)
        cols = pl.ds(i * CHUNK, CHUNK)
        copy = pltpu.make_async_copy(rows.at[:, cols], out_ref.at[:, cols], sent.at[i])
        copy.start()
        leaving.append(copy)
    for copy in leaving:
        copy.wait()


def output_rows(feats, mixes, embed, out_s, out_t):
    tokens, head = feats.shape
    width = embed.shape[1]
    hbm = pl.BlockSpec(memory_space=pl.ANY)
    vmem = pl.BlockSpec(memory_space=pltpu.VMEM)
    return pl.pallas_call(
        output_kernel,
        in_specs=[vmem, vmem, hbm, hbm, hbm],
        out_specs=hbm,
        out_shape=jax.ShapeDtypeStruct((tokens, width), bf16),
        scratch_shapes=[
            pltpu.VMEM((3 * head, width), bf16),
            pltpu.VMEM((tokens, width), bf16),
            pltpu.SemaphoreType.DMA((width // CHUNK, 3)),
            pltpu.SemaphoreType.DMA((width // CHUNK,)),
        ],
        name="output_rows",
    )(feats, mixes, embed, out_s, out_t)


def maps_kernel(at_ref, ws_ref, wt_ref, e_ref, os_ref, gs_ref, gt_ref, maps_ref, e_mine_ref, g_mine_ref):
    rows, triple = ws_ref.shape
    head, wide = e_ref.shape
    first = at_ref[1] * rows
    r = lax.broadcasted_iota(jnp.int32, (rows, wide), 0)
    c = lax.broadcasted_iota(jnp.int32, (rows, wide), 1)
    chosen = jnp.where(c == r + first, 1.0, 0.0)
    pick = chosen.astype(bf16)
    e = e_ref[...]
    e32 = e.astype(f32)
    o32 = os_ref[...].astype(f32)

    def product(weight, scaled):
        placed = tn(weight, pick).astype(bf16)
        high = scaled.astype(bf16)
        low = (scaled - high.astype(f32)).astype(bf16)
        return nt(placed, high) + nt(placed, low)

    gs = gs_ref[...]
    gt = gt_ref[...]
    maps_ref[:triple] = product(ws_ref[...], e32 * gs).astype(bf16)
    later = product(wt_ref[...], jnp.concatenate([e32, o32], axis=0) * gt)
    maps_ref[triple : 2 * triple] = later[:, :head].astype(bf16)
    maps_ref[2 * triple : 3 * triple] = later[:, head:].astype(bf16)
    maps_ref[3 * triple :] = jnp.zeros((maps_ref.shape[0] - 3 * triple, head), bf16)
    e_mine_ref[...] = nt(pick, e).astype(bf16)
    g_mine_ref[...] = jnp.broadcast_to(jnp.sum(chosen * gs, axis=1, keepdims=True), g_mine_ref.shape)


def local_maps(at, w_s, w_t, embed, out_s, gain_s, gain_t, padded):
    rows, triple = w_s.shape
    head, width = embed.shape
    wide = width // lax.axis_size(DP[0]) // lax.axis_size(DP[1])
    full = lambda r, c: pl.BlockSpec((r, c), lambda i, at: (0, 0))
    cut = lambda r: pl.BlockSpec((r, wide), lambda i, at: (0, at[0]))
    return pl.pallas_call(
        maps_kernel,
        grid_spec=pltpu.PrefetchScalarGridSpec(
            num_scalar_prefetch=1,
            grid=(1,),
            in_specs=[full(rows, triple), full(rows, triple), cut(head), cut(head), cut(1), cut(1)],
            out_specs=[full(padded, head), full(rows, head), full(rows, triple)],
        ),
        out_shape=[
            jax.ShapeDtypeStruct((padded, head), bf16),
            jax.ShapeDtypeStruct((rows, head), bf16),
            jax.ShapeDtypeStruct((rows, triple), f32),
        ],
        name="local_maps",
    )(at, w_s, w_t, embed, out_s, gain_s.reshape(1, width), gain_t.reshape(1, width))


def group_size(axes):
    size = 1
    for a in axes:
        size *= lax.axis_size(a)
    return size


def scattered(value):
    n = group_size(PLANE)
    parts = exchange(value.reshape(n, value.shape[0] // n, value.shape[1]), PLANE)
    return parts.astype(f32).sum(axis=0).astype(bf16)


def gathered(mine, shape):
    parts = to_all(mine, LINE)
    mine = parts.astype(f32).sum(axis=0).astype(bf16)
    return to_all(mine, PLANE).reshape(shape)


def softmax_rows(scores):
    top = jnp.max(scores, axis=-1, keepdims=True)
    raised = jnp.exp(scores - top)
    return raised / jnp.sum(raised, axis=-1, keepdims=True)


def attend_kernel(
    at_ref, flat_ref, scaled_ref, gram_ref, cots_ref, maps_ref,
    total_ref, mix_ref, mix_t_ref, qkv_ref, att_ref, dkv_ref, up_ref, score_ref, rounded_ref, slope_ref,
):
    frames = FR
    head = flat_ref.shape[1]
    places = flat_ref.shape[0] // frames
    pad = mix_ref.shape[0] // frames
    triple = 3 * head
    own = frames * pad
    scale = head**-0.5
    line, core, slot, spots = at_ref[0], at_ref[1], at_ref[2], at_ref[3]

    qkv_ref[...] = nt(scaled_ref[...], maps_ref[:triple]).astype(bf16)
    r = lax.broadcasted_iota(jnp.int32, (pad, places), 0)
    c = lax.broadcasted_iota(jnp.int32, (pad, places), 1)
    pick = jnp.where((c == r + slot) & (r < spots), 1.0, 0.0).astype(bf16)

    feats_own, scaled_own, queries = [], [], []
    for f in range(frames):
        here = slice(f * places, (f + 1) * places)
        both = jnp.concatenate([flat_ref[here], scaled_ref[here], qkv_ref[here, :head]], axis=1)
        got = nn(pick, both).astype(bf16)
        feats_own.append(got[:, :head])
        scaled_own.append(got[:, head : 2 * head])
        queries.append(got[:, 2 * head :])
    for f in range(frames):
        here = slice(f * places, (f + 1) * places)
        score_ref[f * pad : (f + 1) * pad] = nt(queries[f], qkv_ref[here, head : 2 * head])
    att = softmax_rows(score_ref[...] * scale)
    att_ref[...] = att
    rounded_ref[...] = att.astype(bf16)
    for f in range(frames):
        here = slice(f * places, (f + 1) * places)
        mine = slice(f * pad, (f + 1) * pad)
        mix_ref[mine] = nn(rounded_ref[mine], qkv_ref[here, 2 * head :]).astype(bf16)

    feats = jnp.concatenate(feats_own, axis=0)
    mix = mix_ref[...]
    x = jnp.concatenate([feats, mix], axis=1)
    gram = gram_ref[...]
    first = gram.astype(bf16)
    rest = gram - first.astype(f32)
    second = rest.astype(bf16)
    third = (rest - second.astype(f32)).astype(bf16)
    xg = nn(x, first) + (nn(x, second) + nn(x, third))
    factor = lax.rsqrt(jnp.sum(xg * x.astype(f32), axis=-1, keepdims=True) + epsilon)
    map_to = maps_ref[2 * triple : 3 * triple]
    raw = nt(feats, maps_ref[triple : 2 * triple]) + nt(mix, map_to)
    packed = (raw * factor).astype(bf16)
    q, k, v = packed[:, :head], packed[:, head : 2 * head], packed[:, 2 * head :]
    g = jnp.concatenate([cots_ref[i, j, 1] for i in range(2) for j in range(4)], axis=0)

    def spot_frame(shape, dim):
        i = lax.broadcasted_iota(jnp.int32, shape, dim)
        f = i // pad
        other = f // 8
        step = (f // 2) % 4
        number = ((line + 4 - step) % 4) * 4 + (core + other - 2 * core * other) * 2 + f % 2
        return i % pad, number

    row_spot, row_frame = spot_frame((own, 1), 0)
    col_spot, col_frame = spot_frame((1, own), 1)
    allowed = (row_spot == col_spot) & (row_frame >= col_frame)
    att = softmax_rows(jnp.where(allowed, nt(q, k) * scale, masked))
    rounded = att.astype(bf16)
    mix_t_ref[...] = nn(rounded, v).astype(bf16)
    d_att = nt(g, v)
    d_sc = (att * (d_att - jnp.sum(d_att * att, axis=-1, keepdims=True))).astype(bf16)
    d_packed = jnp.concatenate(
        [nn(d_sc, k) * scale, tn(d_sc, q) * scale, tn(rounded, g)], axis=1
    ).astype(bf16)
    inner = jnp.sum(d_packed.astype(f32) * raw, axis=-1, keepdims=True)
    corr = factor * nn(d_packed, map_to) - (factor * factor * factor * inner) * xg[:, head:]
    cot = jnp.concatenate([cots_ref[i, j, 0] for i in range(2) for j in range(4)], axis=0)
    up_ref[...] = (cot.astype(f32) + corr).astype(bf16)

    for f in range(frames):
        here = slice(f * places, (f + 1) * places)
        mine = slice(f * pad, (f + 1) * pad)
        score_ref[mine] = nt(up_ref[mine], qkv_ref[here, 2 * head :])
        dkv_ref[here, head:] = tn(rounded_ref[mine], up_ref[mine]).astype(bf16)
    att = att_ref[...]
    d_att = score_ref[...]
    slope_ref[...] = (att * (d_att - jnp.sum(d_att * att, axis=-1, keepdims=True)) * scale).astype(bf16)
    d_queries = []
    for f in range(frames):
        here = slice(f * places, (f + 1) * places)
        mine = slice(f * pad, (f + 1) * pad)
        slope = slope_ref[mine]
        d_queries.append(nn(slope, qkv_ref[here, head : 2 * head]).astype(bf16))
        dkv_ref[here, :head] = tn(slope, queries[f]).astype(bf16)
    by_query = tn(jnp.concatenate(scaled_own, axis=0), jnp.concatenate(d_queries, axis=0))
    by_key = tn(scaled_ref[...], dkv_ref[...])
    total_ref[:head] = by_query.astype(bf16)
    total_ref[head : 2 * head] = by_key[:, :head].astype(bf16)
    total_ref[2 * head : 3 * head] = by_key[:, head:].astype(bf16)
    total_ref[3 * head :] = jnp.zeros((total_ref.shape[0] - 3 * head, head), bf16)


def attend_all(at, flat, scaled, gram, cots, maps, pad):
    rows, head = flat.shape
    places = rows // FR
    own = FR * pad
    vmem = pl.BlockSpec(memory_space=pltpu.VMEM)
    return pl.pallas_call(
        attend_kernel,
        in_specs=[pl.BlockSpec(memory_space=pltpu.SMEM)] + [vmem] * 5,
        out_specs=[vmem] * 3,
        out_shape=[
            jax.ShapeDtypeStruct((4 * head, head), bf16),
            jax.ShapeDtypeStruct((own, head), bf16),
            jax.ShapeDtypeStruct((own, head), bf16),
        ],
        scratch_shapes=[
            pltpu.VMEM((rows, 3 * head), bf16),
            pltpu.VMEM((own, places), f32),
            pltpu.VMEM((rows, 2 * head), bf16),
            pltpu.VMEM((own, head), bf16),
            pltpu.VMEM((own, places), f32),
            pltpu.VMEM((own, places), bf16),
            pltpu.VMEM((own, places), bf16),
        ],
        name="attend_all",
    )(at, flat, scaled, gram, cots, maps)


def turned(value, axis, step):
    n = lax.axis_size(axis)
    return lax.ppermute(value, axis, [(i, (i + step) % n) for i in range(n)])


def shards(
    clip_video,
    conv_weight,
    embed_weight,
    gain_spatial,
    gain_temporal,
    input_spatial,
    input_temporal,
    output_spatial,
    output_temporal,
    cotangent,
):
    frames, height, columns, channels = clip_video.shape
    places = height * columns
    tokens = frames * places
    head, width = embed_weight.shape
    exact = dict(precision=lax.Precision.HIGHEST)
    n_ts = group_size(TS)
    n_clip = group_size(CLIP)
    spots = places // n_clip
    clip_tokens = FR * places

    prior = lax.ppermute(clip_video, TS, [(i, i + 1) for i in range(n_ts - 1)])

    at = jnp.stack([lax.axis_index(DP), lax.axis_index(TS)]).astype(jnp.int32)
    maps, e_mine, g_mine = local_maps(
        at, input_spatial, input_temporal, embed_weight, output_spatial, gain_spatial, gain_temporal, 10 * head
    )
    maps = gathered(scattered(maps), maps.shape)

    feats_home = conv_rows(
        prior.reshape(tokens, channels), clip_video.reshape(tokens, channels), conv_weight
    )
    n_line = lax.axis_size("y")
    line = lax.axis_index("y")
    core = lax.axis_index("c")
    pad = 32
    gram, cots = products(
        embed_weight,
        output_spatial,
        output_temporal,
        cotangent.reshape(tokens, width),
        frames,
        n_clip,
        pad,
    )
    cots = cots.reshape(n_line, 4 * frames * pad, head)
    held = [
        jnp.concatenate(
            [feats_home, lax.dynamic_index_in_dim(cots, (line + step) % n_line, 0, keepdims=False)], axis=0
        )
        for step in range(n_line)
    ]
    moved = []
    for step in range(1, n_line):
        moved.append(turned(held[step], "y", step))
    held = jnp.stack([held[0]] + moved)
    feats_near = held[:, :tokens]
    cots_near = held[:, tokens:].reshape(n_line, 2, 2 * frames * pad, head)
    keep = lax.dynamic_index_in_dim(cots_near, core, 1, keepdims=False)
    give = lax.dynamic_index_in_dim(cots_near, 1 - core, 1, keepdims=False)
    other = turned(jnp.concatenate([feats_near, give], axis=1), "c", 1)
    flat = jnp.concatenate([feats_near, other[:, :tokens]], axis=0).reshape(clip_tokens, head)
    cots = jnp.stack([keep, other[:, tokens:]]).reshape(2, n_line, 2, frames * pad, head)
    wide = flat.astype(f32)
    square = jnp.sum(nn(wide, gram[:head, :head], **exact) * wide, axis=-1, keepdims=True)
    scaled = (wide * lax.rsqrt(square + epsilon)).astype(bf16)

    place = jnp.stack([line, core, lax.axis_index(CLIP) * spots, jnp.int32(spots)]).astype(jnp.int32)
    total, mix, mix_t = attend_all(place, flat, scaled, gram, cots, maps, pad)

    share = scattered(total)
    share, mix, mix_t = lax.optimization_barrier((share, mix, mix_t))
    total = gathered(share, total.shape)
    grad = jnp.concatenate([nn(e_mine, total[b * head : (b + 1) * head]) for b in range(3)], axis=1) * g_mine

    back = jnp.concatenate([mix, mix_t], axis=-1).reshape(2, n_line, frames, pad, 2 * head)[:, :, :, :spots]
    moved = []
    for step in range(1, n_line):
        moved.append(turned(back[:, step], "y", -step))
    back = jnp.stack([back[:, 0]] + moved)
    away = turned(back[:, 1], "c", 1)
    home = jnp.stack([back[:, 0], away], axis=1)
    home = jnp.where(core == 0, home, home[:, ::-1])
    home = lax.dynamic_slice_in_dim(jnp.concatenate([home, home], axis=0), (n_line - line) % n_line, n_line, 0)
    home = home.transpose(2, 0, 1, 3, 4).reshape(tokens, 2 * head)
    layer = output_rows(feats_home, home, embed_weight, output_spatial, output_temporal)
    return (layer.reshape(frames, height, columns, width), grad)


def solution(mesh):
    split = Mesh(mesh.devices.reshape(4, 2, 4, 4, 2), ALL)
    rows = P(ALL, None)
    blocks = P(ALL, None, None, None)
    placed = (blocks, P(), P(), P(), P(), rows, rows, P(), P(), blocks)
    return jax.shard_map(shards, mesh=split, in_specs=placed, out_specs=(blocks, rows), check_vma=False)
```

```python
import jax
import jax.numpy as jnp
from jax import lax
from jax.experimental import pallas as pl
from jax.experimental.pallas import tpu as pltpu
from jax.sharding import Mesh
from jax.sharding import PartitionSpec as P

FR = 16
epsilon = 1e-06
masked = -1e30
f32 = jnp.float32
bf16 = jnp.bfloat16

ALL = ("x", "zh", "zl", "y", "c")
TS = ("zl", "y", "c")
DP = ("x", "zh")
PLANE = ("x", "y", "c")
LINE = ("zh", "zl")
CLIP = ("y", "c")


def nt(a, b, **kw):
    return lax.dot_general(a, b, (((1,), (1,)), ((), ())), preferred_element_type=f32, **kw)


def tn(a, b, **kw):
    return lax.dot_general(a, b, (((0,), (0,)), ((), ())), preferred_element_type=f32, **kw)


def nn(a, b, **kw):
    return lax.dot_general(a, b, (((1,), (0,)), ((), ())), preferred_element_type=f32, **kw)


def exchange(parts, axes):
    return lax.all_to_all(parts, axes, 0, 0, tiled=True)


def to_all(value, axes):
    size = 1
    for a in axes:
        size *= lax.axis_size(a)
    return exchange(jnp.broadcast_to(value, (size,) + value.shape), axes)


def conv_kernel(prior_ref, here_ref, weight_ref, out_ref):
    tokens = here_ref.shape[0]
    columns = here_ref.shape[0] // 8
    volume = jnp.concatenate([prior_ref[...].astype(f32), here_ref[...].astype(f32)], axis=0)
    rows = volume.shape[0]
    place = lax.broadcasted_iota(jnp.int32, (rows, 1), 0) % columns
    left = jnp.where(place == 0, 0.0, pltpu.roll(volume, 1, 0))
    right = jnp.where(place == columns - 1, 0.0, pltpu.roll(volume, rows - 1, 0))
    taps = jnp.concatenate([left, volume, right], axis=1).astype(bf16)
    frame = tokens // 2
    sums = [None, None, None]
    for back in range(3):
        start = (2 - back) * frame
        window = taps[start : start + tokens]
        for up in range(3):
            got = nn(window, weight_ref[back * 3 + up])
            sums[up] = got if sums[up] is None else sums[up] + got
    gap = jnp.zeros((columns, sums[0].shape[1]), f32)
    above, same, below = sums
    for f in range(2):
        lo, hi = f * frame, (f + 1) * frame
        total = (
            same[lo:hi]
            + jnp.concatenate([gap, above[lo : hi - columns]], axis=0)
            + jnp.concatenate([below[lo + columns : hi], gap], axis=0)
        )
        out_ref[lo:hi] = jax.nn.gelu(total, approximate=True).astype(bf16)


def conv_rows(prior, here, weight):
    tokens, channels = here.shape
    vmem = pl.BlockSpec(memory_space=pltpu.VMEM)
    return pl.pallas_call(
        conv_kernel,
        in_specs=[vmem] * 3,
        out_specs=vmem,
        out_shape=jax.ShapeDtypeStruct((tokens, weight.shape[-1]), bf16),
        name="conv_rows",
    )(prior, here, weight.reshape(9, 3 * channels, weight.shape[-1]))


CHUNK = 1024


def products_kernel(
    e_ref, os_ref, ot_ref, cot_ref, gram_ref, cots_ref, weights, cotangents, gram_sum, cots_sum, arrived
):
    head, width = e_ref.shape
    copies = []
    for i in range(width // CHUNK):
        cols = pl.ds(i * CHUNK, CHUNK)
        group = [
            pltpu.make_async_copy(ref.at[:, cols], weights.at[pl.ds(k * head, head), cols], arrived.at[i, k])
            for k, ref in enumerate((e_ref, os_ref, ot_ref))
        ]
        group.append(pltpu.make_async_copy(cot_ref.at[:, cols], cotangents.at[:, cols], arrived.at[i, 3]))
        for copy in group:
            copy.start()
        copies.append(group)
    for i, group in enumerate(copies):
        for copy in group:
            copy.wait()
        cols = slice(i * CHUNK, (i + 1) * CHUNK)
        first = weights[: 2 * head, cols]
        gram = nt(first, first)
        cots = nt(cotangents[:, cols], weights[head:, cols])
        gram_sum[...] = gram if i == 0 else gram_sum[...] + gram
        cots_sum[...] = cots if i == 0 else cots_sum[...] + cots
    gram_ref[...] = gram_sum[...] * (1.0 / width)
    slots, kinds, frames, pad, _ = cots_ref.shape
    places = cots_sum.shape[0] // frames
    spots = places // slots
    r = lax.broadcasted_iota(jnp.int32, (slots * pad, places), 0)
    c = lax.broadcasted_iota(jnp.int32, (slots * pad, places), 1)
    spread = jnp.where((c == (r // pad) * spots + r % pad) & (r % pad < spots), 1.0, 0.0).astype(bf16)
    for f in range(frames):
        got = nn(spread, cots_sum[f * places : (f + 1) * places].astype(bf16)).astype(bf16)
        for slot in range(slots):
            for kind in range(kinds):
                cots_ref[slot, kind, f] = got[slot * pad : (slot + 1) * pad, kind * head : (kind + 1) * head]


def products(embed, out_s, out_t, cot, frames, slots, pad):
    head, width = embed.shape
    tokens = cot.shape[0]
    hbm = pl.BlockSpec(memory_space=pl.ANY)
    vmem = pl.BlockSpec(memory_space=pltpu.VMEM)
    return pl.pallas_call(
        products_kernel,
        in_specs=[hbm] * 4,
        out_specs=[vmem, vmem],
        out_shape=[
            jax.ShapeDtypeStruct((2 * head, 2 * head), f32),
            jax.ShapeDtypeStruct((slots, 2, frames, pad, head), bf16),
        ],
        scratch_shapes=[
            pltpu.VMEM((3 * head, width), bf16),
            pltpu.VMEM((tokens, width), bf16),
            pltpu.VMEM((2 * head, 2 * head), f32),
            pltpu.VMEM((tokens, 2 * head), f32),
            pltpu.SemaphoreType.DMA((width // CHUNK, 4)),
        ],
        name="products",
    )(embed, out_s, out_t, cot)


def output_kernel(f_ref, mixes_ref, e_ref, os_ref, ot_ref, out_ref, weights, rows, arrived, sent):
    head, width = e_ref.shape
    copies = []
    for i in range(width // CHUNK):
        cols = pl.ds(i * CHUNK, CHUNK)
        group = [
            pltpu.make_async_copy(ref.at[:, cols], weights.at[pl.ds(k * head, head), cols], arrived.at[i, k])
            for k, ref in enumerate((e_ref, os_ref, ot_ref))
        ]
        for copy in group:
            copy.start()
        copies.append(group)
    x = jnp.concatenate([f_ref[...], mixes_ref[...]], axis=1)
    leaving = []
    for i, group in enumerate(copies):
        for copy in group:
            copy.wait()
        cols = slice(i * CHUNK, (i + 1) * CHUNK)
        rows[:, cols] = nn(x, weights[:, cols]).astype(bf16)
        cols = pl.ds(i * CHUNK, CHUNK)
        copy = pltpu.make_async_copy(rows.at[:, cols], out_ref.at[:, cols], sent.at[i])
        copy.start()
        leaving.append(copy)
    for copy in leaving:
        copy.wait()


def output_rows(feats, mixes, embed, out_s, out_t):
    tokens, head = feats.shape
    width = embed.shape[1]
    hbm = pl.BlockSpec(memory_space=pl.ANY)
    vmem = pl.BlockSpec(memory_space=pltpu.VMEM)
    return pl.pallas_call(
        output_kernel,
        in_specs=[vmem, vmem, hbm, hbm, hbm],
        out_specs=hbm,
        out_shape=jax.ShapeDtypeStruct((tokens, width), bf16),
        scratch_shapes=[
            pltpu.VMEM((3 * head, width), bf16),
            pltpu.VMEM((tokens, width), bf16),
            pltpu.SemaphoreType.DMA((width // CHUNK, 3)),
            pltpu.SemaphoreType.DMA((width // CHUNK,)),
        ],
        name="output_rows",
    )(feats, mixes, embed, out_s, out_t)


def maps_kernel(
    at_ref, ws_ref, wt_ref, e_ref, os_ref, gs_ref, gt_ref,
    maps_ref, e_mine_ref, g_mine_ref, factors, gains, arrived,
):
    rows, triple = ws_ref.shape
    head = e_ref.shape[0]
    wide = factors.shape[1]
    cols = pl.ds(pl.multiple_of(at_ref[0] * wide, 128), wide)
    copies = [
        pltpu.make_async_copy(e_ref.at[:, cols], factors.at[pl.ds(0, head)], arrived.at[0]),
        pltpu.make_async_copy(os_ref.at[:, cols], factors.at[pl.ds(head, head)], arrived.at[1]),
        pltpu.make_async_copy(gs_ref.at[:, cols], gains.at[0], arrived.at[2]),
        pltpu.make_async_copy(gt_ref.at[:, cols], gains.at[1], arrived.at[3]),
    ]
    for copy in copies:
        copy.start()
    first = at_ref[1] * rows
    r = lax.broadcasted_iota(jnp.int32, (rows, wide), 0)
    c = lax.broadcasted_iota(jnp.int32, (rows, wide), 1)
    chosen = jnp.where(c == r + first, 1.0, 0.0)
    pick = chosen.astype(bf16)
    placed_s = tn(ws_ref[...], pick).astype(bf16)
    placed_t = tn(wt_ref[...], pick).astype(bf16)
    maps_ref[3 * triple :] = jnp.zeros((maps_ref.shape[0] - 3 * triple, head), bf16)
    for copy in copies:
        copy.wait()

    def product(placed, scaled):
        high = scaled.astype(bf16)
        low = (scaled - high.astype(f32)).astype(bf16)
        return nt(placed, high) + nt(placed, low)

    gs = gains[0]
    gt = gains[1]
    both = factors[...].astype(f32)
    maps_ref[:triple] = product(placed_s, both[:head] * gs).astype(bf16)
    later = product(placed_t, both * gt)
    maps_ref[triple : 2 * triple] = later[:, :head].astype(bf16)
    maps_ref[2 * triple : 3 * triple] = later[:, head:].astype(bf16)
    e_mine_ref[...] = nt(pick, factors[:head]).astype(bf16)
    g_mine_ref[...] = jnp.broadcast_to(jnp.sum(chosen * gs, axis=1, keepdims=True), g_mine_ref.shape)


def local_maps(at, w_s, w_t, embed, out_s, gain_s, gain_t, padded):
    rows, triple = w_s.shape
    head, width = embed.shape
    wide = width // lax.axis_size(DP[0]) // lax.axis_size(DP[1])
    hbm = pl.BlockSpec(memory_space=pl.ANY)
    vmem = pl.BlockSpec(memory_space=pltpu.VMEM)
    return pl.pallas_call(
        maps_kernel,
        in_specs=[pl.BlockSpec(memory_space=pltpu.SMEM), vmem, vmem, hbm, hbm, hbm, hbm],
        out_specs=[vmem, vmem, vmem],
        out_shape=[
            jax.ShapeDtypeStruct((padded, head), bf16),
            jax.ShapeDtypeStruct((rows, head), bf16),
            jax.ShapeDtypeStruct((rows, triple), f32),
        ],
        scratch_shapes=[
            pltpu.VMEM((2 * head, wide), bf16),
            pltpu.VMEM((2, 1, wide), f32),
            pltpu.SemaphoreType.DMA((4,)),
        ],
        name="local_maps",
    )(at, w_s, w_t, embed, out_s, gain_s.reshape(1, width), gain_t.reshape(1, width))


def norm_kernel(at_ref, held_ref, one_ref, two_ref, three_ref, other_ref, gram_ref, flat_ref, scaled_ref, cots_ref):
    head = flat_ref.shape[1]
    kinds, span = cots_ref.shape[2], cots_ref.shape[3]
    tokens = other_ref.shape[1] - kinds * span
    gram = gram_ref[:head, :head]
    first = gram.astype(bf16)
    rest = gram - first.astype(f32)
    second = rest.astype(bf16)
    third = (rest - second.astype(f32)).astype(bf16)
    kept = pl.multiple_of(tokens + at_ref[3] * (kinds * span), 16)
    near = (held_ref, one_ref, two_ref, three_ref)
    for side in range(2):
        for step in range(4):
            x = near[step][:tokens] if side == 0 else other_ref[step, :tokens]
            xg = nn(x, first) + (nn(x, second) + nn(x, third))
            wide = x.astype(f32)
            factor = lax.rsqrt(jnp.sum(xg * wide, axis=-1, keepdims=True) + epsilon)
            to = (side * 4 + step) * tokens
            flat_ref[to : to + tokens] = x
            scaled_ref[to : to + tokens] = (wide * factor).astype(bf16)
            if side == 0:
                got = near[step][pl.ds(kept, kinds * span)]
            else:
                got = other_ref[step, tokens:]
            for kind in range(kinds):
                cots_ref[side, step, kind] = got[kind * span : (kind + 1) * span]


def norm_rows(at, near, other, gram, span):
    n_line, rows, head = other.shape
    tokens = rows - 2 * span
    vmem = pl.BlockSpec(memory_space=pltpu.VMEM)
    return pl.pallas_call(
        norm_kernel,
        in_specs=[pl.BlockSpec(memory_space=pltpu.SMEM)] + [vmem] * 6,
        out_specs=[vmem] * 3,
        out_shape=[
            jax.ShapeDtypeStruct((2 * n_line * tokens, head), bf16),
            jax.ShapeDtypeStruct((2 * n_line * tokens, head), bf16),
            jax.ShapeDtypeStruct((2, n_line, 2, span, head), bf16),
        ],
        name="norm_rows",
    )(at, *near, other, gram)


def group_size(axes):
    size = 1
    for a in axes:
        size *= lax.axis_size(a)
    return size


def scattered(value):
    n = group_size(PLANE)
    parts = exchange(value.reshape(n, value.shape[0] // n, value.shape[1]), PLANE)
    return parts.astype(f32).sum(axis=0).astype(bf16)


def gathered(mine, shape):
    parts = to_all(mine, LINE)
    mine = parts.astype(f32).sum(axis=0).astype(bf16)
    return to_all(mine, PLANE).reshape(shape)


def softmax_rows(scores):
    top = jnp.max(scores, axis=-1, keepdims=True)
    raised = jnp.exp(scores - top)
    return raised / jnp.sum(raised, axis=-1, keepdims=True)


def attend_kernel(
    at_ref, flat_ref, scaled_ref, gram_ref, cots_ref, maps_ref,
    total_ref, back_ref, mix_ref, qkv_ref, att_ref, dkv_ref, up_ref, score_ref, rounded_ref, slope_ref,
):
    frames = FR
    head = flat_ref.shape[1]
    places = flat_ref.shape[0] // frames
    pad = mix_ref.shape[0] // frames
    triple = 3 * head
    own = frames * pad
    scale = head**-0.5
    line, core, slot, spots = at_ref[2], at_ref[3], at_ref[4], at_ref[5]

    qkv_ref[...] = nt(scaled_ref[...], maps_ref[:triple]).astype(bf16)
    r = lax.broadcasted_iota(jnp.int32, (pad, places), 0)
    c = lax.broadcasted_iota(jnp.int32, (pad, places), 1)
    pick = jnp.where((c == r + slot) & (r < spots), 1.0, 0.0).astype(bf16)

    feats_own, scaled_own, queries = [], [], []
    for f in range(frames):
        here = slice(f * places, (f + 1) * places)
        both = jnp.concatenate([flat_ref[here], scaled_ref[here], qkv_ref[here, :head]], axis=1)
        got = nn(pick, both).astype(bf16)
        feats_own.append(got[:, :head])
        scaled_own.append(got[:, head : 2 * head])
        queries.append(got[:, 2 * head :])
    for f in range(frames):
        here = slice(f * places, (f + 1) * places)
        score_ref[f * pad : (f + 1) * pad] = nt(queries[f], qkv_ref[here, head : 2 * head])
    att = softmax_rows(score_ref[...] * scale)
    att_ref[...] = att
    rounded_ref[...] = att.astype(bf16)
    for f in range(frames):
        here = slice(f * places, (f + 1) * places)
        mine = slice(f * pad, (f + 1) * pad)
        mix_ref[mine] = nn(rounded_ref[mine], qkv_ref[here, 2 * head :]).astype(bf16)

    feats = jnp.concatenate(feats_own, axis=0)
    mix = mix_ref[...]
    x = jnp.concatenate([feats, mix], axis=1)
    gram = gram_ref[...]
    first = gram.astype(bf16)
    rest = gram - first.astype(f32)
    second = rest.astype(bf16)
    third = (rest - second.astype(f32)).astype(bf16)
    xg = nn(x, first) + (nn(x, second) + nn(x, third))
    factor = lax.rsqrt(jnp.sum(xg * x.astype(f32), axis=-1, keepdims=True) + epsilon)
    map_to = maps_ref[2 * triple : 3 * triple]
    raw = nt(feats, maps_ref[triple : 2 * triple]) + nt(mix, map_to)
    packed = (raw * factor).astype(bf16)
    q, k, v = packed[:, :head], packed[:, head : 2 * head], packed[:, 2 * head :]
    g = jnp.concatenate([cots_ref[i, j, 1] for i in range(2) for j in range(4)], axis=0)

    def spot_frame(shape, dim):
        i = lax.broadcasted_iota(jnp.int32, shape, dim)
        f = i // pad
        other = f // 8
        step = (f // 2) % 4
        number = ((line + 4 - step) % 4) * 4 + (core + other - 2 * core * other) * 2 + f % 2
        return i % pad, number

    row_spot, row_frame = spot_frame((own, 1), 0)
    col_spot, col_frame = spot_frame((1, own), 1)
    allowed = (row_spot == col_spot) & (row_frame >= col_frame)
    att = softmax_rows(jnp.where(allowed, nt(q, k) * scale, masked))
    rounded = att.astype(bf16)
    mix_t = nn(rounded, v).astype(bf16)
    span = back_ref.shape[2]
    for side in range(2):
        for step in range(4):
            mine = slice((side * 4 + step) * span, (side * 4 + step + 1) * span)
            back_ref[step, side] = jnp.concatenate([mix[mine], mix_t[mine]], axis=1)
    d_att = nt(g, v)
    d_sc = (att * (d_att - jnp.sum(d_att * att, axis=-1, keepdims=True))).astype(bf16)
    d_packed = jnp.concatenate(
        [nn(d_sc, k) * scale, tn(d_sc, q) * scale, tn(rounded, g)], axis=1
    ).astype(bf16)
    inner = jnp.sum(d_packed.astype(f32) * raw, axis=-1, keepdims=True)
    corr = factor * nn(d_packed, map_to) - (factor * factor * factor * inner) * xg[:, head:]
    cot = jnp.concatenate([cots_ref[i, j, 0] for i in range(2) for j in range(4)], axis=0)
    up_ref[...] = (cot.astype(f32) + corr).astype(bf16)

    for f in range(frames):
        here = slice(f * places, (f + 1) * places)
        mine = slice(f * pad, (f + 1) * pad)
        score_ref[mine] = nt(up_ref[mine], qkv_ref[here, 2 * head :])
        dkv_ref[here, head:] = tn(rounded_ref[mine], up_ref[mine]).astype(bf16)
    att = att_ref[...]
    d_att = score_ref[...]
    slope_ref[...] = (att * (d_att - jnp.sum(d_att * att, axis=-1, keepdims=True)) * scale).astype(bf16)
    d_queries = []
    for f in range(frames):
        here = slice(f * places, (f + 1) * places)
        mine = slice(f * pad, (f + 1) * pad)
        slope = slope_ref[mine]
        d_queries.append(nn(slope, qkv_ref[here, head : 2 * head]).astype(bf16))
        dkv_ref[here, :head] = tn(slope, queries[f]).astype(bf16)
    by_query = tn(jnp.concatenate(scaled_own, axis=0), jnp.concatenate(d_queries, axis=0))
    by_key = tn(scaled_ref[...], dkv_ref[...])
    total_ref[:head] = by_query.astype(bf16)
    total_ref[head : 2 * head] = by_key[:, :head].astype(bf16)
    total_ref[2 * head : 3 * head] = by_key[:, head:].astype(bf16)
    total_ref[3 * head :] = jnp.zeros((total_ref.shape[0] - 3 * head, head), bf16)


def attend_all(at, flat, scaled, gram, cots, maps, pad):
    rows, head = flat.shape
    places = rows // FR
    own = FR * pad
    vmem = pl.BlockSpec(memory_space=pltpu.VMEM)
    return pl.pallas_call(
        attend_kernel,
        in_specs=[pl.BlockSpec(memory_space=pltpu.SMEM)] + [vmem] * 5,
        out_specs=[vmem] * 2,
        out_shape=[
            jax.ShapeDtypeStruct((4 * head, head), bf16),
            jax.ShapeDtypeStruct((4, 2, own // 8, 2 * head), bf16),
        ],
        scratch_shapes=[
            pltpu.VMEM((own, head), bf16),
            pltpu.VMEM((rows, 3 * head), bf16),
            pltpu.VMEM((own, places), f32),
            pltpu.VMEM((rows, 2 * head), bf16),
            pltpu.VMEM((own, head), bf16),
            pltpu.VMEM((own, places), f32),
            pltpu.VMEM((own, places), bf16),
            pltpu.VMEM((own, places), bf16),
        ],
        name="attend_all",
    )(at, flat, scaled, gram, cots, maps)


def turned(value, axis, step):
    n = lax.axis_size(axis)
    return lax.ppermute(value, axis, [(i, (i + step) % n) for i in range(n)])


def shards(
    clip_video,
    conv_weight,
    embed_weight,
    gain_spatial,
    gain_temporal,
    input_spatial,
    input_temporal,
    output_spatial,
    output_temporal,
    cotangent,
):
    frames, height, columns, channels = clip_video.shape
    places = height * columns
    tokens = frames * places
    head, width = embed_weight.shape
    n_ts = group_size(TS)
    n_clip = group_size(CLIP)
    spots = places // n_clip

    prior = lax.ppermute(clip_video, TS, [(i, i + 1) for i in range(n_ts - 1)])

    n_line = lax.axis_size("y")
    line = lax.axis_index("y")
    core = lax.axis_index("c")
    pad = 32
    at = jnp.stack(
        [lax.axis_index(DP), lax.axis_index(TS), line, core, lax.axis_index(CLIP) * spots, jnp.int32(spots)]
    ).astype(jnp.int32)
    maps, e_mine, g_mine = local_maps(
        at, input_spatial, input_temporal, embed_weight, output_spatial, gain_spatial, gain_temporal, 10 * head
    )
    maps = gathered(scattered(maps), maps.shape)

    feats_home = conv_rows(
        prior.reshape(tokens, channels), clip_video.reshape(tokens, channels), conv_weight
    )
    gram, cots = products(
        embed_weight,
        output_spatial,
        output_temporal,
        cotangent.reshape(tokens, width),
        frames,
        n_clip,
        pad,
    )
    cots = cots.reshape(n_line, 4 * frames * pad, head)
    held = [
        jnp.concatenate(
            [feats_home, lax.dynamic_index_in_dim(cots, (line + step) % n_line, 0, keepdims=False)], axis=0
        )
        for step in range(n_line)
    ]
    moved = []
    for step in range(1, n_line):
        moved.append(turned(held[step], "y", step))
    near = [held[0]] + moved
    span = frames * pad
    give = tokens + (1 - core) * 2 * span
    payload = [
        jnp.concatenate([part[:tokens], lax.dynamic_slice_in_dim(part, give, 2 * span, 0)], axis=0)
        for part in near
    ]
    other = turned(jnp.stack(payload), "c", 1)
    flat, scaled, cots = norm_rows(at, near, other, gram, span)

    total, back = attend_all(at, flat, scaled, gram, cots, maps, pad)
    total = gathered(scattered(total), total.shape)
    grad = jnp.concatenate([nn(e_mine, total[b * head : (b + 1) * head]) for b in range(3)], axis=1) * g_mine

    moved = []
    for step in range(1, n_line):
        moved.append(turned(back[step], "y", -step))
    back = jnp.stack([back[0]] + moved)
    away = turned(back[:, 1], "c", 1)
    home = jnp.stack([back[:, 0], away], axis=1)
    home = jnp.where(core == 0, home, home[:, ::-1])
    home = lax.dynamic_slice_in_dim(jnp.concatenate([home, home], axis=0), (n_line - line) % n_line, n_line, 0)
    home = home.reshape(n_line, 2, frames, pad, 2 * head)[:, :, :, :spots]
    home = home.transpose(2, 0, 1, 3, 4).reshape(tokens, 2 * head)
    layer = output_rows(feats_home, home, embed_weight, output_spatial, output_temporal)
    return (layer.reshape(frames, height, columns, width), grad)


def solution(mesh):
    split = Mesh(mesh.devices.reshape(4, 2, 4, 4, 2), ALL)
    rows = P(ALL, None)
    blocks = P(ALL, None, None, None)
    placed = (blocks, P(), P(), P(), P(), rows, rows, P(), P(), blocks)
    return jax.shard_map(shards, mesh=split, in_specs=placed, out_specs=(blocks, rows), check_vma=False)
```

```python
import jax
import jax.numpy as jnp
from jax import lax
from jax.experimental import pallas as pl
from jax.experimental.pallas import tpu as pltpu
from jax.sharding import Mesh
from jax.sharding import PartitionSpec as P

FR = 16
epsilon = 1e-06
masked = -1e30
f32 = jnp.float32
bf16 = jnp.bfloat16

ALL = ("x", "zh", "zl", "y", "c")
TS = ("zl", "y", "c")
DP = ("x", "zh")
PLANE = ("x", "y", "c")
LINE = ("zh", "zl")
CLIP = ("y", "c")


def nt(a, b, **kw):
    return lax.dot_general(a, b, (((1,), (1,)), ((), ())), preferred_element_type=f32, **kw)


def tn(a, b, **kw):
    return lax.dot_general(a, b, (((0,), (0,)), ((), ())), preferred_element_type=f32, **kw)


def nn(a, b, **kw):
    return lax.dot_general(a, b, (((1,), (0,)), ((), ())), preferred_element_type=f32, **kw)


def exchange(parts, axes):
    return lax.all_to_all(parts, axes, 0, 0, tiled=True)


def to_all(value, axes):
    size = 1
    for a in axes:
        size *= lax.axis_size(a)
    return exchange(jnp.broadcast_to(value, (size,) + value.shape), axes)


def conv_kernel(at_ref, prior_ref, here_ref, weight_ref, cots_ref, own_ref, one_ref, two_ref, three_ref):
    payloads = (own_ref, one_ref, two_ref, three_ref)
    tokens = here_ref.shape[0]
    columns = here_ref.shape[0] // 8
    volume = jnp.concatenate([prior_ref[...].astype(f32), here_ref[...].astype(f32)], axis=0)
    rows = volume.shape[0]
    place = lax.broadcasted_iota(jnp.int32, (rows, 1), 0) % columns
    left = jnp.where(place == 0, 0.0, pltpu.roll(volume, 1, 0))
    right = jnp.where(place == columns - 1, 0.0, pltpu.roll(volume, rows - 1, 0))
    taps = jnp.concatenate([left, volume, right], axis=1).astype(bf16)
    frame = tokens // 2
    sums = [None, None, None]
    for back in range(3):
        start = (2 - back) * frame
        window = taps[start : start + tokens]
        for up in range(3):
            got = nn(window, weight_ref[back * 3 + up])
            sums[up] = got if sums[up] is None else sums[up] + got
    gap = jnp.zeros((columns, sums[0].shape[1]), f32)
    above, same, below = sums
    for f in range(2):
        lo, hi = f * frame, (f + 1) * frame
        total = (
            same[lo:hi]
            + jnp.concatenate([gap, above[lo : hi - columns]], axis=0)
            + jnp.concatenate([below[lo + columns : hi], gap], axis=0)
        )
        feats = jax.nn.gelu(total, approximate=True).astype(bf16)
        for ref in payloads:
            ref[lo:hi] = feats
    for step, ref in enumerate(payloads):
        ref[tokens:] = cots_ref[(at_ref[2] + step) % 4]


def conv_rows(at, prior, here, weight, cots):
    tokens, channels = here.shape
    n_line, extra, head = cots.shape
    vmem = pl.BlockSpec(memory_space=pltpu.VMEM)
    return pl.pallas_call(
        conv_kernel,
        in_specs=[pl.BlockSpec(memory_space=pltpu.SMEM)] + [vmem] * 4,
        out_specs=[vmem] * n_line,
        out_shape=[jax.ShapeDtypeStruct((tokens + extra, head), bf16)] * n_line,
        compiler_params=pltpu.CompilerParams(vmem_limit_bytes=12 << 20),
        name="conv_rows",
    )(at, prior, here, weight.reshape(9, 3 * channels, weight.shape[-1]), cots)


CHUNK = 1024


def products_kernel(
    e_ref, os_ref, ot_ref, cot_ref, gram_ref, cots_ref, weights, cotangents, gram_sum, cots_sum, arrived
):
    head, width = e_ref.shape
    copies = []
    for i in range(width // CHUNK):
        cols = pl.ds(i * CHUNK, CHUNK)
        group = [
            pltpu.make_async_copy(ref.at[:, cols], weights.at[pl.ds(k * head, head), cols], arrived.at[i, k])
            for k, ref in enumerate((e_ref, os_ref, ot_ref))
        ]
        group.append(pltpu.make_async_copy(cot_ref.at[:, cols], cotangents.at[:, cols], arrived.at[i, 3]))
        for copy in group:
            copy.start()
        copies.append(group)
    for i, group in enumerate(copies):
        for copy in group:
            copy.wait()
        cols = slice(i * CHUNK, (i + 1) * CHUNK)
        first = weights[: 2 * head, cols]
        gram = nt(first, first)
        cots = nt(cotangents[:, cols], weights[head:, cols])
        gram_sum[...] = gram if i == 0 else gram_sum[...] + gram
        cots_sum[...] = cots if i == 0 else cots_sum[...] + cots
    gram_ref[...] = gram_sum[...] * (1.0 / width)
    slots, kinds, frames, pad, _ = cots_ref.shape
    places = cots_sum.shape[0] // frames
    spots = places // slots
    r = lax.broadcasted_iota(jnp.int32, (slots * pad, places), 0)
    c = lax.broadcasted_iota(jnp.int32, (slots * pad, places), 1)
    spread = jnp.where((c == (r // pad) * spots + r % pad) & (r % pad < spots), 1.0, 0.0).astype(bf16)
    for f in range(frames):
        got = nn(spread, cots_sum[f * places : (f + 1) * places].astype(bf16)).astype(bf16)
        for slot in range(slots):
            for kind in range(kinds):
                cots_ref[slot, kind, f] = got[slot * pad : (slot + 1) * pad, kind * head : (kind + 1) * head]


def products(embed, out_s, out_t, cot, frames, slots, pad):
    head, width = embed.shape
    tokens = cot.shape[0]
    hbm = pl.BlockSpec(memory_space=pl.ANY)
    vmem = pl.BlockSpec(memory_space=pltpu.VMEM)
    return pl.pallas_call(
        products_kernel,
        in_specs=[hbm] * 4,
        out_specs=[vmem, vmem],
        out_shape=[
            jax.ShapeDtypeStruct((2 * head, 2 * head), f32),
            jax.ShapeDtypeStruct((slots, 2, frames, pad, head), bf16),
        ],
        scratch_shapes=[
            pltpu.VMEM((3 * head, width), bf16),
            pltpu.VMEM((tokens, width), bf16),
            pltpu.VMEM((2 * head, 2 * head), f32),
            pltpu.VMEM((tokens, 2 * head), f32),
            pltpu.SemaphoreType.DMA((width // CHUNK, 4)),
        ],
        name="products",
    )(embed, out_s, out_t, cot)


def output_kernel(f_ref, mixes_ref, e_ref, os_ref, ot_ref, out_ref, weights, rows, arrived, sent):
    head, width = e_ref.shape
    copies = []
    for i in range(width // CHUNK):
        cols = pl.ds(i * CHUNK, CHUNK)
        group = [
            pltpu.make_async_copy(ref.at[:, cols], weights.at[pl.ds(k * head, head), cols], arrived.at[i, k])
            for k, ref in enumerate((e_ref, os_ref, ot_ref))
        ]
        for copy in group:
            copy.start()
        copies.append(group)
    x = jnp.concatenate([f_ref[: rows.shape[0]], mixes_ref[...]], axis=1)
    leaving = []
    for i, group in enumerate(copies):
        for copy in group:
            copy.wait()
        cols = slice(i * CHUNK, (i + 1) * CHUNK)
        rows[:, cols] = nn(x, weights[:, cols]).astype(bf16)
        cols = pl.ds(i * CHUNK, CHUNK)
        copy = pltpu.make_async_copy(rows.at[:, cols], out_ref.at[:, cols], sent.at[i])
        copy.start()
        leaving.append(copy)
    for copy in leaving:
        copy.wait()


def output_rows(feats, mixes, embed, out_s, out_t):
    tokens = mixes.shape[0]
    head, width = embed.shape
    hbm = pl.BlockSpec(memory_space=pl.ANY)
    vmem = pl.BlockSpec(memory_space=pltpu.VMEM)
    return pl.pallas_call(
        output_kernel,
        in_specs=[vmem, vmem, hbm, hbm, hbm],
        out_specs=hbm,
        out_shape=jax.ShapeDtypeStruct((tokens, width), bf16),
        scratch_shapes=[
            pltpu.VMEM((3 * head, width), bf16),
            pltpu.VMEM((tokens, width), bf16),
            pltpu.SemaphoreType.DMA((width // CHUNK, 3)),
            pltpu.SemaphoreType.DMA((width // CHUNK,)),
        ],
        name="output_rows",
    )(feats, mixes, embed, out_s, out_t)


def maps_kernel(
    at_ref, ws_ref, wt_ref, e_ref, os_ref, gs_ref, gt_ref,
    maps_ref, e_mine_ref, g_mine_ref, factors, gains, arrived,
):
    rows, triple = ws_ref.shape
    head = e_ref.shape[0]
    wide = factors.shape[1]
    cols = pl.ds(pl.multiple_of(at_ref[0] * wide, 128), wide)
    copies = [
        pltpu.make_async_copy(e_ref.at[:, cols], factors.at[pl.ds(0, head)], arrived.at[0]),
        pltpu.make_async_copy(os_ref.at[:, cols], factors.at[pl.ds(head, head)], arrived.at[1]),
        pltpu.make_async_copy(gs_ref.at[:, cols], gains.at[0], arrived.at[2]),
        pltpu.make_async_copy(gt_ref.at[:, cols], gains.at[1], arrived.at[3]),
    ]
    for copy in copies:
        copy.start()
    first = at_ref[1] * rows
    r = lax.broadcasted_iota(jnp.int32, (rows, wide), 0)
    c = lax.broadcasted_iota(jnp.int32, (rows, wide), 1)
    chosen = jnp.where(c == r + first, 1.0, 0.0)
    pick = chosen.astype(bf16)
    placed_s = tn(ws_ref[...], pick).astype(bf16)
    placed_t = tn(wt_ref[...], pick).astype(bf16)
    maps_ref[3 * triple :] = jnp.zeros((maps_ref.shape[0] - 3 * triple, head), bf16)
    for copy in copies:
        copy.wait()

    def product(placed, scaled):
        high = scaled.astype(bf16)
        low = (scaled - high.astype(f32)).astype(bf16)
        return nt(placed, high) + nt(placed, low)

    gs = gains[0]
    gt = gains[1]
    both = factors[...].astype(f32)
    maps_ref[:triple] = product(placed_s, both[:head] * gs).astype(bf16)
    later = product(placed_t, both * gt)
    maps_ref[triple : 2 * triple] = later[:, :head].astype(bf16)
    maps_ref[2 * triple : 3 * triple] = later[:, head:].astype(bf16)
    e_mine_ref[...] = nt(pick, factors[:head]).astype(bf16)
    g_mine_ref[...] = jnp.broadcast_to(jnp.sum(chosen * gs, axis=1, keepdims=True), g_mine_ref.shape)


def local_maps(at, w_s, w_t, embed, out_s, gain_s, gain_t, padded):
    rows, triple = w_s.shape
    head, width = embed.shape
    wide = width // lax.axis_size(DP[0]) // lax.axis_size(DP[1])
    hbm = pl.BlockSpec(memory_space=pl.ANY)
    vmem = pl.BlockSpec(memory_space=pltpu.VMEM)
    return pl.pallas_call(
        maps_kernel,
        in_specs=[pl.BlockSpec(memory_space=pltpu.SMEM), vmem, vmem, hbm, hbm, hbm, hbm],
        out_specs=[vmem, vmem, vmem],
        out_shape=[
            jax.ShapeDtypeStruct((padded, head), bf16),
            jax.ShapeDtypeStruct((rows, head), bf16),
            jax.ShapeDtypeStruct((rows, triple), f32),
        ],
        scratch_shapes=[
            pltpu.VMEM((2 * head, wide), bf16),
            pltpu.VMEM((2, 1, wide), f32),
            pltpu.SemaphoreType.DMA((4,)),
        ],
        name="local_maps",
    )(at, w_s, w_t, embed, out_s, gain_s.reshape(1, width), gain_t.reshape(1, width))


def norm_kernel(at_ref, *refs):
    payloads, (gram_ref, flat_ref, scaled_ref, cots_ref) = refs[:8], refs[8:]
    head = flat_ref.shape[1]
    kinds, span = cots_ref.shape[2], cots_ref.shape[3]
    tokens = flat_ref.shape[0] // len(payloads)
    gram = gram_ref[:head, :head]
    first = gram.astype(bf16)
    rest = gram - first.astype(f32)
    second = rest.astype(bf16)
    third = (rest - second.astype(f32)).astype(bf16)
    kept = pl.multiple_of(tokens + at_ref[3] * (kinds * span), 16)
    for i, ref in enumerate(payloads):
        x = ref[:tokens]
        xg = nn(x, first) + (nn(x, second) + nn(x, third))
        wide = x.astype(f32)
        factor = lax.rsqrt(jnp.sum(xg * wide, axis=-1, keepdims=True) + epsilon)
        flat_ref[i * tokens : (i + 1) * tokens] = x
        scaled_ref[i * tokens : (i + 1) * tokens] = (wide * factor).astype(bf16)
        got = ref[pl.ds(kept, kinds * span)]
        for kind in range(kinds):
            cots_ref[i // 4, i % 4, kind] = got[kind * span : (kind + 1) * span]


def norm_rows(at, payloads, gram, span):
    rows, head = payloads[0].shape
    tokens = rows - 4 * span
    vmem = pl.BlockSpec(memory_space=pltpu.VMEM)
    return pl.pallas_call(
        norm_kernel,
        in_specs=[pl.BlockSpec(memory_space=pltpu.SMEM)] + [vmem] * 9,
        out_specs=[vmem] * 3,
        out_shape=[
            jax.ShapeDtypeStruct((8 * tokens, head), bf16),
            jax.ShapeDtypeStruct((8 * tokens, head), bf16),
            jax.ShapeDtypeStruct((2, 4, 2, span, head), bf16),
        ],
        name="norm_rows",
    )(at, *payloads, gram)


def group_size(axes):
    size = 1
    for a in axes:
        size *= lax.axis_size(a)
    return size


def scattered(value):
    n = group_size(PLANE)
    parts = exchange(value.reshape(n, value.shape[0] // n, value.shape[1]), PLANE)
    return parts.astype(f32).sum(axis=0).astype(bf16)


def gathered(mine, shape):
    parts = to_all(mine, LINE)
    mine = parts.astype(f32).sum(axis=0).astype(bf16)
    return to_all(mine, PLANE).reshape(shape)


def softmax_rows(scores):
    top = jnp.max(scores, axis=-1, keepdims=True)
    raised = jnp.exp(scores - top)
    return raised / jnp.sum(raised, axis=-1, keepdims=True)


def attend_kernel(
    at_ref, flat_ref, scaled_ref, gram_ref, cots_ref, maps_ref,
    total_ref, own_ref, one_ref, two_ref, three_ref, mix_ref, qkv_ref, att_ref, dkv_ref, up_ref, score_ref, rounded_ref, slope_ref,
):
    frames = FR
    head = flat_ref.shape[1]
    places = flat_ref.shape[0] // frames
    pad = mix_ref.shape[0] // frames
    triple = 3 * head
    own = frames * pad
    scale = head**-0.5
    line, core, slot, spots = at_ref[2], at_ref[3], at_ref[4], at_ref[5]

    qkv_ref[...] = nt(scaled_ref[...], maps_ref[:triple]).astype(bf16)
    r = lax.broadcasted_iota(jnp.int32, (pad, places), 0)
    c = lax.broadcasted_iota(jnp.int32, (pad, places), 1)
    pick = jnp.where((c == r + slot) & (r < spots), 1.0, 0.0).astype(bf16)

    feats_own, scaled_own, queries = [], [], []
    for f in range(frames):
        here = slice(f * places, (f + 1) * places)
        both = jnp.concatenate([flat_ref[here], scaled_ref[here], qkv_ref[here, :head]], axis=1)
        got = nn(pick, both).astype(bf16)
        feats_own.append(got[:, :head])
        scaled_own.append(got[:, head : 2 * head])
        queries.append(got[:, 2 * head :])
    for f in range(frames):
        here = slice(f * places, (f + 1) * places)
        score_ref[f * pad : (f + 1) * pad] = nt(queries[f], qkv_ref[here, head : 2 * head])
    att = softmax_rows(score_ref[...] * scale)
    att_ref[...] = att
    rounded_ref[...] = att.astype(bf16)
    for f in range(frames):
        here = slice(f * places, (f + 1) * places)
        mine = slice(f * pad, (f + 1) * pad)
        mix_ref[mine] = nn(rounded_ref[mine], qkv_ref[here, 2 * head :]).astype(bf16)

    feats = jnp.concatenate(feats_own, axis=0)
    mix = mix_ref[...]
    x = jnp.concatenate([feats, mix], axis=1)
    gram = gram_ref[...]
    first = gram.astype(bf16)
    rest = gram - first.astype(f32)
    second = rest.astype(bf16)
    third = (rest - second.astype(f32)).astype(bf16)
    xg = nn(x, first) + (nn(x, second) + nn(x, third))
    factor = lax.rsqrt(jnp.sum(xg * x.astype(f32), axis=-1, keepdims=True) + epsilon)
    map_to = maps_ref[2 * triple : 3 * triple]
    raw = nt(feats, maps_ref[triple : 2 * triple]) + nt(mix, map_to)
    packed = (raw * factor).astype(bf16)
    q, k, v = packed[:, :head], packed[:, head : 2 * head], packed[:, 2 * head :]
    g = jnp.concatenate([cots_ref[i, j, 1] for i in range(2) for j in range(4)], axis=0)

    def spot_frame(shape, dim):
        i = lax.broadcasted_iota(jnp.int32, shape, dim)
        f = i // pad
        other = f // 8
        step = (f // 2) % 4
        number = ((line + 4 - step) % 4) * 4 + (core + other - 2 * core * other) * 2 + f % 2
        return i % pad, number

    row_spot, row_frame = spot_frame((own, 1), 0)
    col_spot, col_frame = spot_frame((1, own), 1)
    allowed = (row_spot == col_spot) & (row_frame >= col_frame)
    att = softmax_rows(jnp.where(allowed, nt(q, k) * scale, masked))
    rounded = att.astype(bf16)
    mix_t = nn(rounded, v).astype(bf16)
    span = own_ref.shape[1]
    for side in range(2):
        for step, ref in enumerate((own_ref, one_ref, two_ref, three_ref)):
            mine = slice((side * 4 + step) * span, (side * 4 + step + 1) * span)
            ref[side] = jnp.concatenate([mix[mine], mix_t[mine]], axis=1)
    d_att = nt(g, v)
    d_sc = (att * (d_att - jnp.sum(d_att * att, axis=-1, keepdims=True))).astype(bf16)
    d_packed = jnp.concatenate(
        [nn(d_sc, k) * scale, tn(d_sc, q) * scale, tn(rounded, g)], axis=1
    ).astype(bf16)
    inner = jnp.sum(d_packed.astype(f32) * raw, axis=-1, keepdims=True)
    corr = factor * nn(d_packed, map_to) - (factor * factor * factor * inner) * xg[:, head:]
    cot = jnp.concatenate([cots_ref[i, j, 0] for i in range(2) for j in range(4)], axis=0)
    up_ref[...] = (cot.astype(f32) + corr).astype(bf16)

    for f in range(frames):
        here = slice(f * places, (f + 1) * places)
        mine = slice(f * pad, (f + 1) * pad)
        score_ref[mine] = nt(up_ref[mine], qkv_ref[here, 2 * head :])
        dkv_ref[here, head:] = tn(rounded_ref[mine], up_ref[mine]).astype(bf16)
    att = att_ref[...]
    d_att = score_ref[...]
    slope_ref[...] = (att * (d_att - jnp.sum(d_att * att, axis=-1, keepdims=True)) * scale).astype(bf16)
    d_queries = []
    for f in range(frames):
        here = slice(f * places, (f + 1) * places)
        mine = slice(f * pad, (f + 1) * pad)
        slope = slope_ref[mine]
        d_queries.append(nn(slope, qkv_ref[here, head : 2 * head]).astype(bf16))
        dkv_ref[here, :head] = tn(slope, queries[f]).astype(bf16)
    by_query = tn(jnp.concatenate(scaled_own, axis=0), jnp.concatenate(d_queries, axis=0))
    by_key = tn(scaled_ref[...], dkv_ref[...])
    total_ref[:head] = by_query.astype(bf16)
    total_ref[head : 2 * head] = by_key[:, :head].astype(bf16)
    total_ref[2 * head : 3 * head] = by_key[:, head:].astype(bf16)
    total_ref[3 * head :] = jnp.zeros((total_ref.shape[0] - 3 * head, head), bf16)


def attend_all(at, flat, scaled, gram, cots, maps, pad):
    rows, head = flat.shape
    places = rows // FR
    own = FR * pad
    vmem = pl.BlockSpec(memory_space=pltpu.VMEM)
    return pl.pallas_call(
        attend_kernel,
        in_specs=[pl.BlockSpec(memory_space=pltpu.SMEM)] + [vmem] * 5,
        out_specs=[vmem] * 5,
        out_shape=[jax.ShapeDtypeStruct((4 * head, head), bf16)]
        + [jax.ShapeDtypeStruct((2, own // 8, 2 * head), bf16)] * 4,
        scratch_shapes=[
            pltpu.VMEM((own, head), bf16),
            pltpu.VMEM((rows, 3 * head), bf16),
            pltpu.VMEM((own, places), f32),
            pltpu.VMEM((rows, 2 * head), bf16),
            pltpu.VMEM((own, head), bf16),
            pltpu.VMEM((own, places), f32),
            pltpu.VMEM((own, places), bf16),
            pltpu.VMEM((own, places), bf16),
        ],
        name="attend_all",
    )(at, flat, scaled, gram, cots, maps)


def turned(value, axis, step):
    n = lax.axis_size(axis)
    return lax.ppermute(value, axis, [(i, (i + step) % n) for i in range(n)])


def shards(
    clip_video,
    conv_weight,
    embed_weight,
    gain_spatial,
    gain_temporal,
    input_spatial,
    input_temporal,
    output_spatial,
    output_temporal,
    cotangent,
):
    frames, height, columns, channels = clip_video.shape
    places = height * columns
    tokens = frames * places
    head, width = embed_weight.shape
    n_ts = group_size(TS)
    n_clip = group_size(CLIP)
    spots = places // n_clip

    prior = lax.ppermute(clip_video, TS, [(i, i + 1) for i in range(n_ts - 1)])

    n_line = lax.axis_size("y")
    line = lax.axis_index("y")
    core = lax.axis_index("c")
    pad = 32
    at = jnp.stack(
        [lax.axis_index(DP), lax.axis_index(TS), line, core, lax.axis_index(CLIP) * spots, jnp.int32(spots)]
    ).astype(jnp.int32)
    maps, e_mine, g_mine = local_maps(
        at, input_spatial, input_temporal, embed_weight, output_spatial, gain_spatial, gain_temporal, 10 * head
    )
    maps = gathered(scattered(maps), maps.shape)

    gram, cots = products(
        embed_weight,
        output_spatial,
        output_temporal,
        cotangent.reshape(tokens, width),
        frames,
        n_clip,
        pad,
    )
    cots = cots.reshape(n_line, 4 * frames * pad, head)
    held = conv_rows(
        at, prior.reshape(tokens, channels), clip_video.reshape(tokens, channels), conv_weight, cots
    )
    feats_home = held[0]
    near = [held[0]]
    for step in range(1, n_line):
        near.append(turned(held[step], "y", step))
    other = []
    for step in range(n_line):
        other.append(turned(near[step], "c", 1))
    flat, scaled, cots = norm_rows(at, near + other, gram, frames * pad)

    total, *back = attend_all(at, flat, scaled, gram, cots, maps, pad)
    total = gathered(scattered(total), total.shape)
    grad = jnp.concatenate([nn(e_mine, total[b * head : (b + 1) * head]) for b in range(3)], axis=1) * g_mine

    moved = []
    for step in range(1, n_line):
        moved.append(turned(back[step], "y", -step))
    back = jnp.stack([back[0]] + moved)
    away = turned(back[:, 1], "c", 1)
    home = jnp.stack([back[:, 0], away], axis=1)
    home = jnp.where(core == 0, home, home[:, ::-1])
    home = lax.dynamic_slice_in_dim(jnp.concatenate([home, home], axis=0), (n_line - line) % n_line, n_line, 0)
    home = home.reshape(n_line, 2, frames, pad, 2 * head)[:, :, :, :spots]
    home = home.transpose(2, 0, 1, 3, 4).reshape(tokens, 2 * head)
    layer = output_rows(feats_home, home, embed_weight, output_spatial, output_temporal)
    return (layer.reshape(frames, height, columns, width), grad)


def solution(mesh):
    split = Mesh(mesh.devices.reshape(4, 2, 4, 4, 2), ALL)
    rows = P(ALL, None)
    blocks = P(ALL, None, None, None)
    placed = (blocks, P(), P(), P(), P(), rows, rows, P(), P(), blocks)
    return jax.shard_map(shards, mesh=split, in_specs=placed, out_specs=(blocks, rows), check_vma=False)
```

```python
import jax
import jax.numpy as jnp
from jax import lax
from jax.experimental import pallas as pl
from jax.experimental.pallas import tpu as pltpu
from jax.sharding import Mesh
from jax.sharding import PartitionSpec as P

FR = 16
epsilon = 1e-06
masked = -1e30
f32 = jnp.float32
bf16 = jnp.bfloat16

ALL = ("x", "zh", "zl", "y", "c")
TS = ("zl", "y", "c")
DP = ("x", "zh")
PLANE = ("x", "y", "c")
LINE = ("zh", "zl")
CLIP = ("y", "c")


def nt(a, b, **kw):
    return lax.dot_general(a, b, (((1,), (1,)), ((), ())), preferred_element_type=f32, **kw)


def tn(a, b, **kw):
    return lax.dot_general(a, b, (((0,), (0,)), ((), ())), preferred_element_type=f32, **kw)


def nn(a, b, **kw):
    return lax.dot_general(a, b, (((1,), (0,)), ((), ())), preferred_element_type=f32, **kw)


def exchange(parts, axes):
    return lax.all_to_all(parts, axes, 0, 0, tiled=True)


def to_all(value, axes):
    size = 1
    for a in axes:
        size *= lax.axis_size(a)
    return exchange(jnp.broadcast_to(value, (size,) + value.shape), axes)


def conv_kernel(at_ref, prior_ref, here_ref, weight_ref, cots_ref, own_ref, one_ref, two_ref, three_ref):
    payloads = (own_ref, one_ref, two_ref, three_ref)
    tokens = here_ref.shape[0]
    columns = here_ref.shape[0] // 8
    volume = jnp.concatenate([prior_ref[...].astype(f32), here_ref[...].astype(f32)], axis=0)
    rows = volume.shape[0]
    place = lax.broadcasted_iota(jnp.int32, (rows, 1), 0) % columns
    left = jnp.where(place == 0, 0.0, pltpu.roll(volume, 1, 0))
    right = jnp.where(place == columns - 1, 0.0, pltpu.roll(volume, rows - 1, 0))
    taps = jnp.concatenate([left, volume, right], axis=1).astype(bf16)
    frame = tokens // 2
    sums = [None, None, None]
    for back in range(3):
        start = (2 - back) * frame
        window = taps[start : start + tokens]
        for up in range(3):
            got = nn(window, weight_ref[back * 3 + up])
            sums[up] = got if sums[up] is None else sums[up] + got
    gap = jnp.zeros((columns, sums[0].shape[1]), f32)
    above, same, below = sums
    for f in range(2):
        lo, hi = f * frame, (f + 1) * frame
        total = (
            same[lo:hi]
            + jnp.concatenate([gap, above[lo : hi - columns]], axis=0)
            + jnp.concatenate([below[lo + columns : hi], gap], axis=0)
        )
        feats = jax.nn.gelu(total, approximate=True).astype(bf16)
        for ref in payloads:
            ref[lo:hi] = feats
    for step, ref in enumerate(payloads):
        ref[tokens:] = cots_ref[(at_ref[2] + step) % 4]


def conv_rows(at, prior, here, weight, cots):
    tokens, channels = here.shape
    n_line, extra, head = cots.shape
    vmem = pl.BlockSpec(memory_space=pltpu.VMEM)
    return pl.pallas_call(
        conv_kernel,
        in_specs=[pl.BlockSpec(memory_space=pltpu.SMEM)] + [vmem] * 4,
        out_specs=[vmem] * n_line,
        out_shape=[jax.ShapeDtypeStruct((tokens + extra, head), bf16)] * n_line,
        compiler_params=pltpu.CompilerParams(vmem_limit_bytes=12 << 20),
        name="conv_rows",
    )(at, prior, here, weight.reshape(9, 3 * channels, weight.shape[-1]), cots)


CHUNK = 1024


def products_kernel(
    e_ref, os_ref, ot_ref, cot_ref, gram_ref, cots_ref, weights, cotangents, gram_sum, cots_sum, arrived
):
    head, width = e_ref.shape
    copies = []
    for i in range(width // CHUNK):
        cols = pl.ds(i * CHUNK, CHUNK)
        group = [
            pltpu.make_async_copy(ref.at[:, cols], weights.at[pl.ds(k * head, head), cols], arrived.at[i, k])
            for k, ref in enumerate((e_ref, os_ref, ot_ref))
        ]
        group.append(pltpu.make_async_copy(cot_ref.at[:, cols], cotangents.at[:, cols], arrived.at[i, 3]))
        for copy in group:
            copy.start()
        copies.append(group)
    for i, group in enumerate(copies):
        for copy in group:
            copy.wait()
        cols = slice(i * CHUNK, (i + 1) * CHUNK)
        first = weights[: 2 * head, cols]
        gram = nt(first, first)
        cots = nt(cotangents[:, cols], weights[head:, cols])
        gram_sum[...] = gram if i == 0 else gram_sum[...] + gram
        cots_sum[...] = cots if i == 0 else cots_sum[...] + cots
    gram_ref[...] = gram_sum[...] * (1.0 / width)
    slots, kinds, frames, pad, _ = cots_ref.shape
    places = cots_sum.shape[0] // frames
    spots = places // slots
    r = lax.broadcasted_iota(jnp.int32, (slots * pad, places), 0)
    c = lax.broadcasted_iota(jnp.int32, (slots * pad, places), 1)
    spread = jnp.where((c == (r // pad) * spots + r % pad) & (r % pad < spots), 1.0, 0.0).astype(bf16)
    for f in range(frames):
        got = nn(spread, cots_sum[f * places : (f + 1) * places].astype(bf16)).astype(bf16)
        for slot in range(slots):
            for kind in range(kinds):
                cots_ref[slot, kind, f] = got[slot * pad : (slot + 1) * pad, kind * head : (kind + 1) * head]


def products(embed, out_s, out_t, cot, frames, slots, pad):
    head, width = embed.shape
    tokens = cot.shape[0]
    hbm = pl.BlockSpec(memory_space=pl.ANY)
    vmem = pl.BlockSpec(memory_space=pltpu.VMEM)
    return pl.pallas_call(
        products_kernel,
        in_specs=[hbm] * 4,
        out_specs=[vmem, vmem],
        out_shape=[
            jax.ShapeDtypeStruct((2 * head, 2 * head), f32),
            jax.ShapeDtypeStruct((slots, 2, frames, pad, head), bf16),
        ],
        scratch_shapes=[
            pltpu.VMEM((3 * head, width), bf16),
            pltpu.VMEM((tokens, width), bf16),
            pltpu.VMEM((2 * head, 2 * head), f32),
            pltpu.VMEM((tokens, 2 * head), f32),
            pltpu.SemaphoreType.DMA((width // CHUNK, 4)),
        ],
        name="products",
    )(embed, out_s, out_t, cot)


def output_kernel(at_ref, f_ref, *refs):
    parts = refs[:8]
    e_ref, os_ref, ot_ref, out_ref, weights, rows, arrived, sent = refs[8:]
    head, width = e_ref.shape
    copies = []
    for i in range(width // CHUNK):
        cols = pl.ds(i * CHUNK, CHUNK)
        group = [
            pltpu.make_async_copy(ref.at[:, cols], weights.at[pl.ds(k * head, head), cols], arrived.at[i, k])
            for k, ref in enumerate((e_ref, os_ref, ot_ref))
        ]
        for copy in group:
            copy.start()
        copies.append(group)
    line, core, spots = at_ref[2], at_ref[3], at_ref[5]
    tokens = rows.shape[0]
    places = tokens // 2
    pad = parts[0].shape[1] // 2
    r = lax.broadcasted_iota(jnp.int32, (places, 8 * pad), 0)
    c = lax.broadcasted_iota(jnp.int32, (places, 8 * pad), 1)
    step = (c // pad) % 4
    side = c // (4 * pad)
    slot = ((line + step) % 4) * 2 + core + side - 2 * core * side
    place = jnp.where((r == slot * spots + c % pad) & (c % pad < spots), 1.0, 0.0).astype(bf16)
    mixes = []
    for f in range(2):
        got = jnp.concatenate([ref[i // 4, f * pad : (f + 1) * pad] for i, ref in enumerate(parts)], axis=0)
        mixes.append(nn(place, got).astype(bf16))
    x = jnp.concatenate([f_ref[:tokens], jnp.concatenate(mixes, axis=0)], axis=1)
    leaving = []
    for i, group in enumerate(copies):
        for copy in group:
            copy.wait()
        cols = slice(i * CHUNK, (i + 1) * CHUNK)
        rows[:, cols] = nn(x, weights[:, cols]).astype(bf16)
        cols = pl.ds(i * CHUNK, CHUNK)
        copy = pltpu.make_async_copy(rows.at[:, cols], out_ref.at[:, cols], sent.at[i])
        copy.start()
        leaving.append(copy)
    for copy in leaving:
        copy.wait()


def output_rows(at, feats, parts, embed, out_s, out_t, tokens):
    head, width = embed.shape
    hbm = pl.BlockSpec(memory_space=pl.ANY)
    vmem = pl.BlockSpec(memory_space=pltpu.VMEM)
    return pl.pallas_call(
        output_kernel,
        in_specs=[pl.BlockSpec(memory_space=pltpu.SMEM)] + [vmem] * 9 + [hbm] * 3,
        out_specs=hbm,
        out_shape=jax.ShapeDtypeStruct((tokens, width), bf16),
        scratch_shapes=[
            pltpu.VMEM((3 * head, width), bf16),
            pltpu.VMEM((tokens, width), bf16),
            pltpu.SemaphoreType.DMA((width // CHUNK, 3)),
            pltpu.SemaphoreType.DMA((width // CHUNK,)),
        ],
        name="output_rows",
    )(at, feats, *parts, embed, out_s, out_t)


def maps_kernel(
    at_ref, ws_ref, wt_ref, e_ref, os_ref, gs_ref, gt_ref,
    maps_ref, e_mine_ref, g_mine_ref, factors, gains, projections, arrived,
):
    rows, triple = ws_ref.shape
    head = e_ref.shape[0]
    wide = factors.shape[1]
    cols = pl.ds(pl.multiple_of(at_ref[0] * wide, 128), wide)
    copies = [
        pltpu.make_async_copy(ws_ref, projections.at[0], arrived.at[4]),
        pltpu.make_async_copy(wt_ref, projections.at[1], arrived.at[5]),
        pltpu.make_async_copy(e_ref.at[:, cols], factors.at[pl.ds(0, head)], arrived.at[0]),
        pltpu.make_async_copy(os_ref.at[:, cols], factors.at[pl.ds(head, head)], arrived.at[1]),
        pltpu.make_async_copy(gs_ref.at[:, cols], gains.at[0], arrived.at[2]),
        pltpu.make_async_copy(gt_ref.at[:, cols], gains.at[1], arrived.at[3]),
    ]
    for copy in copies:
        copy.start()
    first = at_ref[1] * rows
    r = lax.broadcasted_iota(jnp.int32, (rows, wide), 0)
    c = lax.broadcasted_iota(jnp.int32, (rows, wide), 1)
    chosen = jnp.where(c == r + first, 1.0, 0.0)
    pick = chosen.astype(bf16)
    maps_ref[3 * triple :] = jnp.zeros((maps_ref.shape[0] - 3 * triple, head), bf16)
    for copy in copies:
        copy.wait()
    placed_s = tn(projections[0], pick).astype(bf16)
    placed_t = tn(projections[1], pick).astype(bf16)

    def product(placed, scaled):
        high = scaled.astype(bf16)
        low = (scaled - high.astype(f32)).astype(bf16)
        return nt(placed, high) + nt(placed, low)

    gs = gains[0]
    gt = gains[1]
    both = factors[...].astype(f32)
    maps_ref[:triple] = product(placed_s, both[:head] * gs).astype(bf16)
    later = product(placed_t, both * gt)
    maps_ref[triple : 2 * triple] = later[:, :head].astype(bf16)
    maps_ref[2 * triple : 3 * triple] = later[:, head:].astype(bf16)
    e_mine_ref[...] = nt(pick, factors[:head]).astype(bf16)
    g_mine_ref[...] = jnp.broadcast_to(jnp.sum(chosen * gs, axis=1, keepdims=True), g_mine_ref.shape)


def local_maps(at, w_s, w_t, embed, out_s, gain_s, gain_t, padded):
    rows, triple = w_s.shape
    head, width = embed.shape
    wide = width // lax.axis_size(DP[0]) // lax.axis_size(DP[1])
    hbm = pl.BlockSpec(memory_space=pl.ANY)
    vmem = pl.BlockSpec(memory_space=pltpu.VMEM)
    return pl.pallas_call(
        maps_kernel,
        in_specs=[pl.BlockSpec(memory_space=pltpu.SMEM)] + [hbm] * 6,
        out_specs=[vmem, vmem, vmem],
        out_shape=[
            jax.ShapeDtypeStruct((padded, head), bf16),
            jax.ShapeDtypeStruct((rows, head), bf16),
            jax.ShapeDtypeStruct((rows, triple), f32),
        ],
        scratch_shapes=[
            pltpu.VMEM((2 * head, wide), bf16),
            pltpu.VMEM((2, 1, wide), f32),
            pltpu.VMEM((2, rows, triple), bf16),
            pltpu.SemaphoreType.DMA((6,)),
        ],
        name="local_maps",
    )(at, w_s, w_t, embed, out_s, gain_s.reshape(1, width), gain_t.reshape(1, width))


def norm_kernel(at_ref, *refs):
    payloads, (gram_ref, flat_ref, scaled_ref, cots_ref) = refs[:8], refs[8:]
    head = flat_ref.shape[1]
    kinds, span = cots_ref.shape[2], cots_ref.shape[3]
    tokens = flat_ref.shape[0] // len(payloads)
    gram = gram_ref[:head, :head]
    first = gram.astype(bf16)
    rest = gram - first.astype(f32)
    second = rest.astype(bf16)
    third = (rest - second.astype(f32)).astype(bf16)
    kept = pl.multiple_of(tokens + at_ref[3] * (kinds * span), 16)
    for i, ref in enumerate(payloads):
        x = ref[:tokens]
        xg = nn(x, first) + (nn(x, second) + nn(x, third))
        wide = x.astype(f32)
        factor = lax.rsqrt(jnp.sum(xg * wide, axis=-1, keepdims=True) + epsilon)
        flat_ref[i * tokens : (i + 1) * tokens] = x
        scaled_ref[i * tokens : (i + 1) * tokens] = (wide * factor).astype(bf16)
        got = ref[pl.ds(kept, kinds * span)]
        for kind in range(kinds):
            cots_ref[i // 4, i % 4, kind] = got[kind * span : (kind + 1) * span]


def norm_rows(at, payloads, gram, span):
    rows, head = payloads[0].shape
    tokens = rows - 4 * span
    vmem = pl.BlockSpec(memory_space=pltpu.VMEM)
    return pl.pallas_call(
        norm_kernel,
        in_specs=[pl.BlockSpec(memory_space=pltpu.SMEM)] + [vmem] * 9,
        out_specs=[vmem] * 3,
        out_shape=[
            jax.ShapeDtypeStruct((8 * tokens, head), bf16),
            jax.ShapeDtypeStruct((8 * tokens, head), bf16),
            jax.ShapeDtypeStruct((2, 4, 2, span, head), bf16),
        ],
        name="norm_rows",
    )(at, *payloads, gram)


def group_size(axes):
    size = 1
    for a in axes:
        size *= lax.axis_size(a)
    return size


def scattered(value):
    n = group_size(PLANE)
    parts = exchange(value.reshape(n, value.shape[0] // n, value.shape[1]), PLANE)
    return parts.astype(f32).sum(axis=0).astype(bf16)


def gathered(mine, shape):
    parts = to_all(mine, LINE)
    mine = parts.astype(f32).sum(axis=0).astype(bf16)
    return to_all(mine, PLANE).reshape(shape)


def softmax_rows(scores):
    top = jnp.max(scores, axis=-1, keepdims=True)
    raised = jnp.exp(scores - top)
    return raised / jnp.sum(raised, axis=-1, keepdims=True)


def attend_kernel(
    at_ref, flat_ref, scaled_ref, gram_ref, cots_ref, maps_ref,
    total_ref, own_ref, one_ref, two_ref, three_ref, mix_ref, qkv_ref, att_ref, dkv_ref, up_ref, score_ref, rounded_ref, slope_ref,
):
    frames = FR
    head = flat_ref.shape[1]
    places = flat_ref.shape[0] // frames
    pad = mix_ref.shape[0] // frames
    triple = 3 * head
    own = frames * pad
    scale = head**-0.5
    line, core, slot, spots = at_ref[2], at_ref[3], at_ref[4], at_ref[5]

    qkv_ref[...] = nt(scaled_ref[...], maps_ref[:triple]).astype(bf16)
    r = lax.broadcasted_iota(jnp.int32, (pad, places), 0)
    c = lax.broadcasted_iota(jnp.int32, (pad, places), 1)
    pick = jnp.where((c == r + slot) & (r < spots), 1.0, 0.0).astype(bf16)

    feats_own, scaled_own, queries = [], [], []
    for f in range(frames):
        here = slice(f * places, (f + 1) * places)
        both = jnp.concatenate([flat_ref[here], scaled_ref[here], qkv_ref[here, :head]], axis=1)
        got = nn(pick, both).astype(bf16)
        feats_own.append(got[:, :head])
        scaled_own.append(got[:, head : 2 * head])
        queries.append(got[:, 2 * head :])
    for f in range(frames):
        here = slice(f * places, (f + 1) * places)
        score_ref[f * pad : (f + 1) * pad] = nt(queries[f], qkv_ref[here, head : 2 * head])
    att = softmax_rows(score_ref[...] * scale)
    att_ref[...] = att
    rounded_ref[...] = att.astype(bf16)
    for f in range(frames):
        here = slice(f * places, (f + 1) * places)
        mine = slice(f * pad, (f + 1) * pad)
        mix_ref[mine] = nn(rounded_ref[mine], qkv_ref[here, 2 * head :]).astype(bf16)

    feats = jnp.concatenate(feats_own, axis=0)
    mix = mix_ref[...]
    x = jnp.concatenate([feats, mix], axis=1)
    gram = gram_ref[...]
    first = gram.astype(bf16)
    rest = gram - first.astype(f32)
    second = rest.astype(bf16)
    third = (rest - second.astype(f32)).astype(bf16)
    xg = nn(x, first) + (nn(x, second) + nn(x, third))
    factor = lax.rsqrt(jnp.sum(xg * x.astype(f32), axis=-1, keepdims=True) + epsilon)
    map_to = maps_ref[2 * triple : 3 * triple]
    raw = nt(feats, maps_ref[triple : 2 * triple]) + nt(mix, map_to)
    packed = (raw * factor).astype(bf16)
    q, k, v = packed[:, :head], packed[:, head : 2 * head], packed[:, 2 * head :]
    g = jnp.concatenate([cots_ref[i, j, 1] for i in range(2) for j in range(4)], axis=0)

    def spot_frame(shape, dim):
        i = lax.broadcasted_iota(jnp.int32, shape, dim)
        f = i // pad
        other = f // 8
        step = (f // 2) % 4
        number = ((line + 4 - step) % 4) * 4 + (core + other - 2 * core * other) * 2 + f % 2
        return i % pad, number

    row_spot, row_frame = spot_frame((own, 1), 0)
    col_spot, col_frame = spot_frame((1, own), 1)
    allowed = (row_spot == col_spot) & (row_frame >= col_frame)
    att = softmax_rows(jnp.where(allowed, nt(q, k) * scale, masked))
    rounded = att.astype(bf16)
    mix_t = nn(rounded, v).astype(bf16)
    span = own_ref.shape[1]
    for side in range(2):
        for step, ref in enumerate((own_ref, one_ref, two_ref, three_ref)):
            mine = slice((side * 4 + step) * span, (side * 4 + step + 1) * span)
            ref[side] = jnp.concatenate([mix[mine], mix_t[mine]], axis=1)
    d_att = nt(g, v)
    d_sc = (att * (d_att - jnp.sum(d_att * att, axis=-1, keepdims=True))).astype(bf16)
    d_packed = jnp.concatenate(
        [nn(d_sc, k) * scale, tn(d_sc, q) * scale, tn(rounded, g)], axis=1
    ).astype(bf16)
    inner = jnp.sum(d_packed.astype(f32) * raw, axis=-1, keepdims=True)
    corr = factor * nn(d_packed, map_to) - (factor * factor * factor * inner) * xg[:, head:]
    cot = jnp.concatenate([cots_ref[i, j, 0] for i in range(2) for j in range(4)], axis=0)
    up_ref[...] = (cot.astype(f32) + corr).astype(bf16)

    for f in range(frames):
        here = slice(f * places, (f + 1) * places)
        mine = slice(f * pad, (f + 1) * pad)
        score_ref[mine] = nt(up_ref[mine], qkv_ref[here, 2 * head :])
        dkv_ref[here, head:] = tn(rounded_ref[mine], up_ref[mine]).astype(bf16)
    att = att_ref[...]
    d_att = score_ref[...]
    slope_ref[...] = (att * (d_att - jnp.sum(d_att * att, axis=-1, keepdims=True)) * scale).astype(bf16)
    d_queries = []
    for f in range(frames):
        here = slice(f * places, (f + 1) * places)
        mine = slice(f * pad, (f + 1) * pad)
        slope = slope_ref[mine]
        d_queries.append(nn(slope, qkv_ref[here, head : 2 * head]).astype(bf16))
        dkv_ref[here, :head] = tn(slope, queries[f]).astype(bf16)
    by_query = tn(jnp.concatenate(scaled_own, axis=0), jnp.concatenate(d_queries, axis=0))
    by_key = tn(scaled_ref[...], dkv_ref[...])
    total_ref[:head] = by_query.astype(bf16)
    total_ref[head : 2 * head] = by_key[:, :head].astype(bf16)
    total_ref[2 * head : 3 * head] = by_key[:, head:].astype(bf16)
    total_ref[3 * head :] = jnp.zeros((total_ref.shape[0] - 3 * head, head), bf16)


def attend_all(at, flat, scaled, gram, cots, maps, pad):
    rows, head = flat.shape
    places = rows // FR
    own = FR * pad
    vmem = pl.BlockSpec(memory_space=pltpu.VMEM)
    return pl.pallas_call(
        attend_kernel,
        in_specs=[pl.BlockSpec(memory_space=pltpu.SMEM)] + [vmem] * 5,
        out_specs=[vmem] * 5,
        out_shape=[jax.ShapeDtypeStruct((4 * head, head), bf16)]
        + [jax.ShapeDtypeStruct((2, own // 8, 2 * head), bf16)] * 4,
        scratch_shapes=[
            pltpu.VMEM((own, head), bf16),
            pltpu.VMEM((rows, 3 * head), bf16),
            pltpu.VMEM((own, places), f32),
            pltpu.VMEM((rows, 2 * head), bf16),
            pltpu.VMEM((own, head), bf16),
            pltpu.VMEM((own, places), f32),
            pltpu.VMEM((own, places), bf16),
            pltpu.VMEM((own, places), bf16),
        ],
        name="attend_all",
    )(at, flat, scaled, gram, cots, maps)


def turned(value, axis, step):
    n = lax.axis_size(axis)
    return lax.ppermute(value, axis, [(i, (i + step) % n) for i in range(n)])


def shards(
    clip_video,
    conv_weight,
    embed_weight,
    gain_spatial,
    gain_temporal,
    input_spatial,
    input_temporal,
    output_spatial,
    output_temporal,
    cotangent,
):
    frames, height, columns, channels = clip_video.shape
    places = height * columns
    tokens = frames * places
    head, width = embed_weight.shape
    n_ts = group_size(TS)
    n_clip = group_size(CLIP)
    spots = places // n_clip

    prior = lax.ppermute(clip_video, TS, [(i, i + 1) for i in range(n_ts - 1)])

    n_line = lax.axis_size("y")
    line = lax.axis_index("y")
    core = lax.axis_index("c")
    pad = 32
    at = jnp.stack(
        [lax.axis_index(DP), lax.axis_index(TS), line, core, lax.axis_index(CLIP) * spots, jnp.int32(spots)]
    ).astype(jnp.int32)
    maps, e_mine, g_mine = local_maps(
        at, input_spatial, input_temporal, embed_weight, output_spatial, gain_spatial, gain_temporal, 10 * head
    )
    maps = gathered(scattered(maps), maps.shape)

    gram, cots = products(
        embed_weight,
        output_spatial,
        output_temporal,
        cotangent.reshape(tokens, width),
        frames,
        n_clip,
        pad,
    )
    cots = cots.reshape(n_line, 4 * frames * pad, head)
    held = conv_rows(
        at, prior.reshape(tokens, channels), clip_video.reshape(tokens, channels), conv_weight, cots
    )
    feats_home = held[0]
    near = [held[0]]
    for step in range(1, n_line):
        near.append(turned(held[step], "y", step))
    other = []
    for step in range(n_line):
        other.append(turned(near[step], "c", 1))
    flat, scaled, cots = norm_rows(at, near + other, gram, frames * pad)

    total, *back = attend_all(at, flat, scaled, gram, cots, maps, pad)
    total = gathered(scattered(total), total.shape)
    grad = jnp.concatenate([nn(e_mine, total[b * head : (b + 1) * head]) for b in range(3)], axis=1) * g_mine

    near = [back[0]]
    for step in range(1, n_line):
        near.append(turned(back[step], "y", -step))
    other = []
    for step in range(n_line):
        other.append(turned(near[step], "c", 1))
    layer = output_rows(at, feats_home, near + other, embed_weight, output_spatial, output_temporal, tokens)
    return (layer.reshape(frames, height, columns, width), grad)


def solution(mesh):
    split = Mesh(mesh.devices.reshape(4, 2, 4, 4, 2), ALL)
    rows = P(ALL, None)
    blocks = P(ALL, None, None, None)
    placed = (blocks, P(), P(), P(), P(), rows, rows, P(), P(), blocks)
    return jax.shard_map(shards, mesh=split, in_specs=placed, out_specs=(blocks, rows), check_vma=False)
```

```python
import jax
import jax.numpy as jnp
from jax import lax
from jax.experimental import pallas as pl
from jax.experimental.pallas import tpu as pltpu
from jax.sharding import Mesh
from jax.sharding import PartitionSpec as P

FR = 16
epsilon = 1e-06
masked = -1e30
f32 = jnp.float32
bf16 = jnp.bfloat16

ALL = ("x", "zh", "zl", "y", "c")
TS = ("zl", "y", "c")
DP = ("x", "zh")
PLANE = ("x", "y", "c")
LINE = ("zh", "zl")
CLIP = ("y", "c")


def nt(a, b, **kw):
    return lax.dot_general(a, b, (((1,), (1,)), ((), ())), preferred_element_type=f32, **kw)


def tn(a, b, **kw):
    return lax.dot_general(a, b, (((0,), (0,)), ((), ())), preferred_element_type=f32, **kw)


def nn(a, b, **kw):
    return lax.dot_general(a, b, (((1,), (0,)), ((), ())), preferred_element_type=f32, **kw)


def exchange(parts, axes):
    return lax.all_to_all(parts, axes, 0, 0, tiled=True)


def to_all(value, axes):
    size = 1
    for a in axes:
        size *= lax.axis_size(a)
    return exchange(jnp.broadcast_to(value, (size,) + value.shape), axes)


def conv_kernel(at_ref, prior_ref, here_ref, weight_ref, cots_ref, own_ref, one_ref, two_ref, three_ref):
    payloads = (own_ref, one_ref, two_ref, three_ref)
    tokens = here_ref.shape[0]
    columns = here_ref.shape[0] // 8
    volume = jnp.concatenate([prior_ref[...].astype(f32), here_ref[...].astype(f32)], axis=0)
    rows = volume.shape[0]
    place = lax.broadcasted_iota(jnp.int32, (rows, 1), 0) % columns
    left = jnp.where(place == 0, 0.0, pltpu.roll(volume, 1, 0))
    right = jnp.where(place == columns - 1, 0.0, pltpu.roll(volume, rows - 1, 0))
    taps = jnp.concatenate([left, volume, right], axis=1).astype(bf16)
    frame = tokens // 2
    sums = [None, None, None]
    for back in range(3):
        start = (2 - back) * frame
        window = taps[start : start + tokens]
        for up in range(3):
            got = nn(window, weight_ref[back * 3 + up])
            sums[up] = got if sums[up] is None else sums[up] + got
    gap = jnp.zeros((columns, sums[0].shape[1]), f32)
    above, same, below = sums
    for f in range(2):
        lo, hi = f * frame, (f + 1) * frame
        total = (
            same[lo:hi]
            + jnp.concatenate([gap, above[lo : hi - columns]], axis=0)
            + jnp.concatenate([below[lo + columns : hi], gap], axis=0)
        )
        feats = jax.nn.gelu(total, approximate=True).astype(bf16)
        for ref in payloads:
            ref[lo:hi] = feats
    for step, ref in enumerate(payloads):
        ref[tokens:] = cots_ref[(at_ref[2] + step) % 4]


def conv_rows(at, prior, here, weight, cots):
    tokens, channels = here.shape
    n_line, extra, head = cots.shape
    vmem = pl.BlockSpec(memory_space=pltpu.VMEM)
    return pl.pallas_call(
        conv_kernel,
        in_specs=[pl.BlockSpec(memory_space=pltpu.SMEM)] + [vmem] * 4,
        out_specs=[vmem] * n_line,
        out_shape=[jax.ShapeDtypeStruct((tokens + extra, head), bf16)] * n_line,
        compiler_params=pltpu.CompilerParams(vmem_limit_bytes=12 << 20),
        name="conv_rows",
    )(at, prior, here, weight.reshape(9, 3 * channels, weight.shape[-1]), cots)


CHUNK = 1024


def products_kernel(
    e_ref, os_ref, ot_ref, cot_ref, gram_ref, cots_ref, weights, cotangents, gram_sum, cots_sum, arrived
):
    head, width = e_ref.shape
    copies = []
    for i in range(width // CHUNK):
        cols = pl.ds(i * CHUNK, CHUNK)
        group = [
            pltpu.make_async_copy(ref.at[:, cols], weights.at[pl.ds(k * head, head), cols], arrived.at[i, k])
            for k, ref in enumerate((e_ref, os_ref, ot_ref))
        ]
        group.append(pltpu.make_async_copy(cot_ref.at[:, cols], cotangents.at[:, cols], arrived.at[i, 3]))
        for copy in group:
            copy.start()
        copies.append(group)
    for i, group in enumerate(copies):
        for copy in group:
            copy.wait()
        cols = slice(i * CHUNK, (i + 1) * CHUNK)
        first = weights[: 2 * head, cols]
        gram = nt(first, first)
        cots = nt(cotangents[:, cols], weights[head:, cols])
        gram_sum[...] = gram if i == 0 else gram_sum[...] + gram
        cots_sum[...] = cots if i == 0 else cots_sum[...] + cots
    gram_ref[...] = gram_sum[...] * (1.0 / width)
    slots, kinds, frames, pad, _ = cots_ref.shape
    places = cots_sum.shape[0] // frames
    spots = places // slots
    r = lax.broadcasted_iota(jnp.int32, (slots * pad, places), 0)
    c = lax.broadcasted_iota(jnp.int32, (slots * pad, places), 1)
    spread = jnp.where((c == (r // pad) * spots + r % pad) & (r % pad < spots), 1.0, 0.0).astype(bf16)
    for f in range(frames):
        got = nn(spread, cots_sum[f * places : (f + 1) * places].astype(bf16)).astype(bf16)
        for slot in range(slots):
            for kind in range(kinds):
                cots_ref[slot, kind, f] = got[slot * pad : (slot + 1) * pad, kind * head : (kind + 1) * head]


def products(embed, out_s, out_t, cot, frames, slots, pad):
    head, width = embed.shape
    tokens = cot.shape[0]
    hbm = pl.BlockSpec(memory_space=pl.ANY)
    vmem = pl.BlockSpec(memory_space=pltpu.VMEM)
    return pl.pallas_call(
        products_kernel,
        in_specs=[hbm] * 4,
        out_specs=[vmem, vmem],
        out_shape=[
            jax.ShapeDtypeStruct((2 * head, 2 * head), f32),
            jax.ShapeDtypeStruct((slots, 2, frames, pad, head), bf16),
        ],
        scratch_shapes=[
            pltpu.VMEM((3 * head, width), bf16),
            pltpu.VMEM((tokens, width), bf16),
            pltpu.VMEM((2 * head, 2 * head), f32),
            pltpu.VMEM((tokens, 2 * head), f32),
            pltpu.SemaphoreType.DMA((width // CHUNK, 4)),
        ],
        name="products",
    )(embed, out_s, out_t, cot)


SLAB = 640


def output_kernel(at_ref, f_ref, *refs):
    parts = refs[:8]
    e_ref, os_ref, ot_ref, out_ref, weights, rows, arrived, sent = refs[8:]
    head, width = e_ref.shape
    copies = []
    for i in range(width // SLAB):
        cols = pl.ds(i * SLAB, SLAB)
        group = [
            pltpu.make_async_copy(ref.at[:, cols], weights.at[pl.ds(k * head, head), cols], arrived.at[i, k])
            for k, ref in enumerate((e_ref, os_ref, ot_ref))
        ]
        for copy in group:
            copy.start()
        copies.append(group)
    line, core, spots = at_ref[2], at_ref[3], at_ref[5]
    tokens = rows.shape[0]
    places = tokens // 2
    pad = parts[0].shape[1] // 2
    r = lax.broadcasted_iota(jnp.int32, (places, 8 * pad), 0)
    c = lax.broadcasted_iota(jnp.int32, (places, 8 * pad), 1)
    step = (c // pad) % 4
    side = c // (4 * pad)
    slot = ((line + step) % 4) * 2 + core + side - 2 * core * side
    place = jnp.where((r == slot * spots + c % pad) & (c % pad < spots), 1.0, 0.0).astype(bf16)
    mixes = []
    for f in range(2):
        got = jnp.concatenate([ref[i // 4, f * pad : (f + 1) * pad] for i, ref in enumerate(parts)], axis=0)
        mixes.append(nn(place, got).astype(bf16))
    x = jnp.concatenate([f_ref[:tokens], jnp.concatenate(mixes, axis=0)], axis=1)
    leaving = []
    for i, group in enumerate(copies):
        for copy in group:
            copy.wait()
        cols = slice(i * SLAB, (i + 1) * SLAB)
        rows[:, cols] = nn(x, weights[:, cols]).astype(bf16)
        cols = pl.ds(i * SLAB, SLAB)
        copy = pltpu.make_async_copy(rows.at[:, cols], out_ref.at[:, cols], sent.at[i])
        copy.start()
        leaving.append(copy)
    for copy in leaving:
        copy.wait()


def output_rows(at, feats, parts, embed, out_s, out_t, tokens):
    head, width = embed.shape
    hbm = pl.BlockSpec(memory_space=pl.ANY)
    vmem = pl.BlockSpec(memory_space=pltpu.VMEM)
    return pl.pallas_call(
        output_kernel,
        in_specs=[pl.BlockSpec(memory_space=pltpu.SMEM)] + [vmem] * 9 + [hbm] * 3,
        out_specs=hbm,
        out_shape=jax.ShapeDtypeStruct((tokens, width), bf16),
        scratch_shapes=[
            pltpu.VMEM((3 * head, width), bf16),
            pltpu.VMEM((tokens, width), bf16),
            pltpu.SemaphoreType.DMA((width // SLAB, 3)),
            pltpu.SemaphoreType.DMA((width // SLAB,)),
        ],
        compiler_params=pltpu.CompilerParams(vmem_limit_bytes=12 << 20),
        name="output_rows",
    )(at, feats, *parts, embed, out_s, out_t)


def maps_kernel(
    at_ref, ws_ref, wt_ref, e_ref, os_ref, gs_ref, gt_ref,
    maps_ref, e_mine_ref, g_mine_ref, factors, gains, projections, arrived,
):
    rows, triple = ws_ref.shape
    head = e_ref.shape[0]
    wide = factors.shape[1]
    cols = pl.ds(pl.multiple_of(at_ref[0] * wide, 128), wide)
    copies = [
        pltpu.make_async_copy(ws_ref, projections.at[0], arrived.at[4]),
        pltpu.make_async_copy(wt_ref, projections.at[1], arrived.at[5]),
        pltpu.make_async_copy(e_ref.at[:, cols], factors.at[pl.ds(0, head)], arrived.at[0]),
        pltpu.make_async_copy(os_ref.at[:, cols], factors.at[pl.ds(head, head)], arrived.at[1]),
        pltpu.make_async_copy(gs_ref.at[:, cols], gains.at[0], arrived.at[2]),
        pltpu.make_async_copy(gt_ref.at[:, cols], gains.at[1], arrived.at[3]),
    ]
    for copy in copies:
        copy.start()
    first = at_ref[1] * rows
    r = lax.broadcasted_iota(jnp.int32, (rows, wide), 0)
    c = lax.broadcasted_iota(jnp.int32, (rows, wide), 1)
    chosen = jnp.where(c == r + first, 1.0, 0.0)
    pick = chosen.astype(bf16)
    maps_ref[3 * triple :] = jnp.zeros((maps_ref.shape[0] - 3 * triple, head), bf16)
    for copy in copies:
        copy.wait()
    placed_s = tn(projections[0], pick).astype(bf16)
    placed_t = tn(projections[1], pick).astype(bf16)

    def product(placed, scaled):
        high = scaled.astype(bf16)
        low = (scaled - high.astype(f32)).astype(bf16)
        return nt(placed, high) + nt(placed, low)

    gs = gains[0]
    gt = gains[1]
    both = factors[...].astype(f32)
    maps_ref[:triple] = product(placed_s, both[:head] * gs).astype(bf16)
    later = product(placed_t, both * gt)
    maps_ref[triple : 2 * triple] = later[:, :head].astype(bf16)
    maps_ref[2 * triple : 3 * triple] = later[:, head:].astype(bf16)
    e_mine_ref[...] = nt(pick, factors[:head]).astype(bf16)
    g_mine_ref[...] = jnp.broadcast_to(jnp.sum(chosen * gs, axis=1, keepdims=True), g_mine_ref.shape)


def local_maps(at, w_s, w_t, embed, out_s, gain_s, gain_t, padded):
    rows, triple = w_s.shape
    head, width = embed.shape
    wide = width // lax.axis_size(DP[0]) // lax.axis_size(DP[1])
    hbm = pl.BlockSpec(memory_space=pl.ANY)
    vmem = pl.BlockSpec(memory_space=pltpu.VMEM)
    return pl.pallas_call(
        maps_kernel,
        in_specs=[pl.BlockSpec(memory_space=pltpu.SMEM)] + [hbm] * 6,
        out_specs=[vmem, vmem, vmem],
        out_shape=[
            jax.ShapeDtypeStruct((padded, head), bf16),
            jax.ShapeDtypeStruct((rows, head), bf16),
            jax.ShapeDtypeStruct((rows, triple), f32),
        ],
        scratch_shapes=[
            pltpu.VMEM((2 * head, wide), bf16),
            pltpu.VMEM((2, 1, wide), f32),
            pltpu.VMEM((2, rows, triple), bf16),
            pltpu.SemaphoreType.DMA((6,)),
        ],
        name="local_maps",
    )(at, w_s, w_t, embed, out_s, gain_s.reshape(1, width), gain_t.reshape(1, width))


def norm_kernel(at_ref, *refs):
    payloads, (gram_ref, flat_ref, scaled_ref, cots_ref) = refs[:8], refs[8:]
    head = flat_ref.shape[1]
    kinds, span = cots_ref.shape[2], cots_ref.shape[3]
    tokens = flat_ref.shape[0] // len(payloads)
    gram = gram_ref[:head, :head]
    first = gram.astype(bf16)
    rest = gram - first.astype(f32)
    second = rest.astype(bf16)
    third = (rest - second.astype(f32)).astype(bf16)
    kept = pl.multiple_of(tokens + at_ref[3] * (kinds * span), 16)
    for i, ref in enumerate(payloads):
        x = ref[:tokens]
        xg = nn(x, first) + (nn(x, second) + nn(x, third))
        wide = x.astype(f32)
        factor = lax.rsqrt(jnp.sum(xg * wide, axis=-1, keepdims=True) + epsilon)
        flat_ref[i * tokens : (i + 1) * tokens] = x
        scaled_ref[i * tokens : (i + 1) * tokens] = (wide * factor).astype(bf16)
        got = ref[pl.ds(kept, kinds * span)]
        for kind in range(kinds):
            cots_ref[i // 4, i % 4, kind] = got[kind * span : (kind + 1) * span]


def norm_rows(at, payloads, gram, span):
    rows, head = payloads[0].shape
    tokens = rows - 4 * span
    vmem = pl.BlockSpec(memory_space=pltpu.VMEM)
    return pl.pallas_call(
        norm_kernel,
        in_specs=[pl.BlockSpec(memory_space=pltpu.SMEM)] + [vmem] * 9,
        out_specs=[vmem] * 3,
        out_shape=[
            jax.ShapeDtypeStruct((8 * tokens, head), bf16),
            jax.ShapeDtypeStruct((8 * tokens, head), bf16),
            jax.ShapeDtypeStruct((2, 4, 2, span, head), bf16),
        ],
        name="norm_rows",
    )(at, *payloads, gram)


def group_size(axes):
    size = 1
    for a in axes:
        size *= lax.axis_size(a)
    return size


def scattered(value):
    n = group_size(PLANE)
    parts = exchange(value.reshape(n, value.shape[0] // n, value.shape[1]), PLANE)
    return parts.astype(f32).sum(axis=0).astype(bf16)


def gathered(mine, shape):
    parts = to_all(mine, LINE)
    mine = parts.astype(f32).sum(axis=0).astype(bf16)
    return to_all(mine, PLANE).reshape(shape)


def softmax_rows(scores):
    top = jnp.max(scores, axis=-1, keepdims=True)
    raised = jnp.exp(scores - top)
    return raised / jnp.sum(raised, axis=-1, keepdims=True)


def attend_kernel(
    at_ref, flat_ref, scaled_ref, gram_ref, cots_ref, maps_ref,
    total_ref, own_ref, one_ref, two_ref, three_ref, mix_ref, qkv_ref, att_ref, dkv_ref, up_ref, score_ref, rounded_ref, slope_ref,
):
    frames = FR
    head = flat_ref.shape[1]
    places = flat_ref.shape[0] // frames
    pad = mix_ref.shape[0] // frames
    triple = 3 * head
    own = frames * pad
    scale = head**-0.5
    line, core, slot, spots = at_ref[2], at_ref[3], at_ref[4], at_ref[5]

    qkv_ref[...] = nt(scaled_ref[...], maps_ref[:triple]).astype(bf16)
    r = lax.broadcasted_iota(jnp.int32, (pad, places), 0)
    c = lax.broadcasted_iota(jnp.int32, (pad, places), 1)
    pick = jnp.where((c == r + slot) & (r < spots), 1.0, 0.0).astype(bf16)

    feats_own, scaled_own, queries = [], [], []
    for f in range(frames):
        here = slice(f * places, (f + 1) * places)
        both = jnp.concatenate([flat_ref[here], scaled_ref[here], qkv_ref[here, :head]], axis=1)
        got = nn(pick, both).astype(bf16)
        feats_own.append(got[:, :head])
        scaled_own.append(got[:, head : 2 * head])
        queries.append(got[:, 2 * head :])
    for f in range(frames):
        here = slice(f * places, (f + 1) * places)
        score_ref[f * pad : (f + 1) * pad] = nt(queries[f], qkv_ref[here, head : 2 * head])
    att = softmax_rows(score_ref[...] * scale)
    att_ref[...] = att
    rounded_ref[...] = att.astype(bf16)
    for f in range(frames):
        here = slice(f * places, (f + 1) * places)
        mine = slice(f * pad, (f + 1) * pad)
        mix_ref[mine] = nn(rounded_ref[mine], qkv_ref[here, 2 * head :]).astype(bf16)

    feats = jnp.concatenate(feats_own, axis=0)
    mix = mix_ref[...]
    x = jnp.concatenate([feats, mix], axis=1)
    gram = gram_ref[...]
    first = gram.astype(bf16)
    rest = gram - first.astype(f32)
    second = rest.astype(bf16)
    third = (rest - second.astype(f32)).astype(bf16)
    xg = nn(x, first) + (nn(x, second) + nn(x, third))
    factor = lax.rsqrt(jnp.sum(xg * x.astype(f32), axis=-1, keepdims=True) + epsilon)
    map_to = maps_ref[2 * triple : 3 * triple]
    raw = nt(feats, maps_ref[triple : 2 * triple]) + nt(mix, map_to)
    packed = (raw * factor).astype(bf16)
    q, k, v = packed[:, :head], packed[:, head : 2 * head], packed[:, 2 * head :]
    g = jnp.concatenate([cots_ref[i, j, 1] for i in range(2) for j in range(4)], axis=0)

    def spot_frame(shape, dim):
        i = lax.broadcasted_iota(jnp.int32, shape, dim)
        f = i // pad
        other = f // 8
        step = (f // 2) % 4
        number = ((line + 4 - step) % 4) * 4 + (core + other - 2 * core * other) * 2 + f % 2
        return i % pad, number

    row_spot, row_frame = spot_frame((own, 1), 0)
    col_spot, col_frame = spot_frame((1, own), 1)
    allowed = (row_spot == col_spot) & (row_frame >= col_frame)
    att = softmax_rows(jnp.where(allowed, nt(q, k) * scale, masked))
    rounded = att.astype(bf16)
    mix_t = nn(rounded, v).astype(bf16)
    span = own_ref.shape[1]
    for side in range(2):
        for step, ref in enumerate((own_ref, one_ref, two_ref, three_ref)):
            mine = slice((side * 4 + step) * span, (side * 4 + step + 1) * span)
            ref[side] = jnp.concatenate([mix[mine], mix_t[mine]], axis=1)
    d_att = nt(g, v)
    d_sc = (att * (d_att - jnp.sum(d_att * att, axis=-1, keepdims=True))).astype(bf16)
    d_packed = jnp.concatenate(
        [nn(d_sc, k) * scale, tn(d_sc, q) * scale, tn(rounded, g)], axis=1
    ).astype(bf16)
    inner = jnp.sum(d_packed.astype(f32) * raw, axis=-1, keepdims=True)
    corr = factor * nn(d_packed, map_to) - (factor * factor * factor * inner) * xg[:, head:]
    cot = jnp.concatenate([cots_ref[i, j, 0] for i in range(2) for j in range(4)], axis=0)
    up_ref[...] = (cot.astype(f32) + corr).astype(bf16)

    for f in range(frames):
        here = slice(f * places, (f + 1) * places)
        mine = slice(f * pad, (f + 1) * pad)
        score_ref[mine] = nt(up_ref[mine], qkv_ref[here, 2 * head :])
        dkv_ref[here, head:] = tn(rounded_ref[mine], up_ref[mine]).astype(bf16)
    att = att_ref[...]
    d_att = score_ref[...]
    slope_ref[...] = (att * (d_att - jnp.sum(d_att * att, axis=-1, keepdims=True)) * scale).astype(bf16)
    d_queries = []
    for f in range(frames):
        here = slice(f * places, (f + 1) * places)
        mine = slice(f * pad, (f + 1) * pad)
        slope = slope_ref[mine]
        d_queries.append(nn(slope, qkv_ref[here, head : 2 * head]).astype(bf16))
        dkv_ref[here, :head] = tn(slope, queries[f]).astype(bf16)
    by_query = tn(jnp.concatenate(scaled_own, axis=0), jnp.concatenate(d_queries, axis=0))
    by_key = tn(scaled_ref[...], dkv_ref[...])
    total_ref[:head] = by_query.astype(bf16)
    total_ref[head : 2 * head] = by_key[:, :head].astype(bf16)
    total_ref[2 * head : 3 * head] = by_key[:, head:].astype(bf16)
    total_ref[3 * head :] = jnp.zeros((total_ref.shape[0] - 3 * head, head), bf16)


def attend_all(at, flat, scaled, gram, cots, maps, pad):
    rows, head = flat.shape
    places = rows // FR
    own = FR * pad
    vmem = pl.BlockSpec(memory_space=pltpu.VMEM)
    return pl.pallas_call(
        attend_kernel,
        in_specs=[pl.BlockSpec(memory_space=pltpu.SMEM)] + [vmem] * 5,
        out_specs=[vmem] * 5,
        out_shape=[jax.ShapeDtypeStruct((4 * head, head), bf16)]
        + [jax.ShapeDtypeStruct((2, own // 8, 2 * head), bf16)] * 4,
        scratch_shapes=[
            pltpu.VMEM((own, head), bf16),
            pltpu.VMEM((rows, 3 * head), bf16),
            pltpu.VMEM((own, places), f32),
            pltpu.VMEM((rows, 2 * head), bf16),
            pltpu.VMEM((own, head), bf16),
            pltpu.VMEM((own, places), f32),
            pltpu.VMEM((own, places), bf16),
            pltpu.VMEM((own, places), bf16),
        ],
        name="attend_all",
    )(at, flat, scaled, gram, cots, maps)


def turned(value, axis, step):
    n = lax.axis_size(axis)
    return lax.ppermute(value, axis, [(i, (i + step) % n) for i in range(n)])


def shards(
    clip_video,
    conv_weight,
    embed_weight,
    gain_spatial,
    gain_temporal,
    input_spatial,
    input_temporal,
    output_spatial,
    output_temporal,
    cotangent,
):
    frames, height, columns, channels = clip_video.shape
    places = height * columns
    tokens = frames * places
    head, width = embed_weight.shape
    n_ts = group_size(TS)
    n_clip = group_size(CLIP)
    spots = places // n_clip

    prior = lax.ppermute(clip_video, TS, [(i, i + 1) for i in range(n_ts - 1)])

    n_line = lax.axis_size("y")
    line = lax.axis_index("y")
    core = lax.axis_index("c")
    pad = 32
    at = jnp.stack(
        [lax.axis_index(DP), lax.axis_index(TS), line, core, lax.axis_index(CLIP) * spots, jnp.int32(spots)]
    ).astype(jnp.int32)
    maps, e_mine, g_mine = local_maps(
        at, input_spatial, input_temporal, embed_weight, output_spatial, gain_spatial, gain_temporal, 10 * head
    )
    maps = gathered(scattered(maps), maps.shape)

    gram, cots = products(
        embed_weight,
        output_spatial,
        output_temporal,
        cotangent.reshape(tokens, width),
        frames,
        n_clip,
        pad,
    )
    cots = cots.reshape(n_line, 4 * frames * pad, head)
    held = conv_rows(
        at, prior.reshape(tokens, channels), clip_video.reshape(tokens, channels), conv_weight, cots
    )
    feats_home = held[0]
    near = [held[0]]
    for step in range(1, n_line):
        near.append(turned(held[step], "y", step))
    other = []
    for step in range(n_line):
        other.append(turned(near[step], "c", 1))
    flat, scaled, cots = norm_rows(at, near + other, gram, frames * pad)

    total, *back = attend_all(at, flat, scaled, gram, cots, maps, pad)
    total = gathered(scattered(total), total.shape)
    grad = jnp.concatenate([nn(e_mine, total[b * head : (b + 1) * head]) for b in range(3)], axis=1) * g_mine

    near = [back[0]]
    for step in range(1, n_line):
        near.append(turned(back[step], "y", -step))
    other = []
    for step in range(n_line):
        other.append(turned(near[step], "c", 1))
    layer = output_rows(at, feats_home, near + other, embed_weight, output_spatial, output_temporal, tokens)
    return (layer.reshape(frames, height, columns, width), grad)


def solution(mesh):
    split = Mesh(mesh.devices.reshape(4, 2, 4, 4, 2), ALL)
    rows = P(ALL, None)
    blocks = P(ALL, None, None, None)
    placed = (blocks, P(), P(), P(), P(), rows, rows, P(), P(), blocks)
    return jax.shard_map(shards, mesh=split, in_specs=placed, out_specs=(blocks, rows), check_vma=False)
```
